128 devices in a mesh: row: 16 (over z, x), col: 8 (over y, core).
Axes of the slice: x: 4, y: 4, z: 4, core: 2. Of those that a mesh axis runs over, the one named last changes fastest.
Arguments:
- density_first: bfloat16 [12288, 12288], P('row', 'col'), may hold values from -0.0068359375 to 0.0068359375
- density_second: bfloat16 [12288, 12288], P('row', 'col'), may hold values from -0.0068359375 to 0.0068359375
- basis: bfloat16 [256, 4096, 896], P(('row', 'col')), may hold values from -6 to 6
- tile_list: int32 [256, 7], P(('row', 'col')), may hold values from 0 to 95, as said below
- tile_count: int32 [256], P(('row', 'col')), may hold values from 5 to 7, as said below
- point_count: int32 [256], P(('row', 'col')), may hold values from 1024 to 4096, as said below
- offsets: float32 [3, 256, 4096], P(None, ('row', 'col')), may hold values from -5 to 5
- weights: float32 [256, 4096], P(('row', 'col')), may hold values from 0.05 to 1
- atom_of_point: int32 [256, 4096], P(('row', 'col')), may hold values from 0 to 1023, as said below
Outputs:
- density: float32 [2, 256, 4096], P(None, ('row', 'col'))
- moments: float32 [2, 9, 1024], replicated
The draws below stay inside these ranges and needn't reach their ends.
Inputs may be any that keep to these rules, and one draw needn't show every extreme that they name: `tile_list`: the 7 tile numbers of each batch are 7 consecutive numbers in some order. `tile_count`: some batch has 7. `point_count`: some batch has 4096. `atom_of_point`: the points of batch g belong to atoms (g * 4 + j) mod 1024 with j from 0 to 7.
All inputs are finite; a program needn't handle non-finite values.
Results may differ from the reference program's by a relative error of at most 0.0003.
Values may be sent and summed in bfloat16 or wider, within the bound.
No kernel may reach another device: no remote copies, remote signals or barrier semaphores. Data moves between devices by JAX's collectives and lax.ppermute only.
A program may use at most 192 MiB of HBM per device.

```python
import math
import jax
import jax.numpy as jnp
from jax import lax

TILE = 128
NB = 12288
KT = 7
PTS = 4096
ATOMS = 1024
NT = 96
BATCHES = 256
N_ROW = 16
N_COL = 8


def lift_one(key, values, top):
    chosen = jax.random.randint(jax.random.fold_in(key, 17), (), 0, values.shape[0])
    return jnp.where(jnp.arange(values.shape[0]) == chosen, top, values).astype(jnp.int32)


def draw_tile_list(key, part):
    start_key = jax.random.fold_in(key, 3)
    order_key = jax.random.fold_in(key, 5)
    starts = jax.random.randint(start_key, (BATCHES, 1), 0, NT - KT + 1)
    order_keys = jax.random.split(order_key, BATCHES)
    orders = jax.vmap(lambda single: jax.random.permutation(single, KT))(order_keys)
    return (starts + orders).astype(jnp.int32)


def draw_tile_count(key, part):
    base = jax.random.randint(jax.random.fold_in(key, 7), (BATCHES,), KT - 2, KT + 1)
    return lift_one(key, base, KT)


def draw_point_count(key, part):
    base = jax.random.randint(jax.random.fold_in(key, 11), (BATCHES,), PTS // 4, PTS + 1)
    return lift_one(key, base, PTS)


def draw_atom_of_point(key, part):
    base = (jnp.arange(BATCHES, dtype=jnp.int32) * ATOMS // BATCHES)[:, None]
    spread = jax.random.randint(jax.random.fold_in(key, 13), (BATCHES, PTS), 0, 8)
    return ((base + spread) % ATOMS).astype(jnp.int32)


def level_of(own_key, extent, pieces, low, largest):
    def one(dim, blocks):
        steps = jax.random.uniform(jax.random.fold_in(jax.random.fold_in(own_key, 6), dim), (blocks,), jnp.float32, low / len(pieces), largest / len(pieces))
        return jnp.repeat(jnp.exp(steps), extent[dim] // blocks).reshape((-1,) + (1,) * (len(extent) - dim - 1))

    gain = one(*pieces[0])
    for cut in pieces[1:]:
        gain = gain * one(*cut)
    return gain


def normal_values(key, dims, scale, reach, pieces=(), kind=jnp.bfloat16):
    entries = jax.random.normal(key, dims, jnp.float32) * scale
    if len(pieces) > 0:
        entries = level_of(key, dims, pieces, -0.22, 0.18) * entries
    return jnp.clip(entries, min=-reach, max=reach).astype(kind)


def setup_inputs(seed: int = 0) -> dict:
    seeds = jax.random.split(jax.random.key(seed), 10)
    density_first = normal_values(seeds[0], (NB, NB), ((KT * TILE) ** 2) ** -0.5, 0.0068359375, ((0, 16), (1, 8)))
    density_second = normal_values(seeds[1], (NB, NB), ((KT * TILE) ** 2) ** -0.5, 0.0068359375, ((0, 16), (1, 8)))
    basis = normal_values(seeds[2], (BATCHES, PTS, KT * TILE), 1.0, 6.0, ((0, 128),))
    tile_list = draw_tile_list(jax.random.fold_in(seeds[9], 71), 0)
    tile_count = draw_tile_count(jax.random.fold_in(seeds[9], 71), 0)
    point_count = draw_point_count(jax.random.fold_in(seeds[9], 71), 0)
    offsets = normal_values(seeds[6], (3, BATCHES, PTS), 1.0, 5.0, ((1, 128),), jnp.float32)
    weights = jnp.clip(jnp.exp(math.log(1.0) - 2.9957323 * jax.random.uniform(seeds[7], (BATCHES, PTS), jnp.float32) ** level_of(seeds[7], (BATCHES, PTS), ((0, 128),), -0.2, 0.2)), 0.05, 1.0)
    atom_of_point = draw_atom_of_point(jax.random.fold_in(seeds[9], 71), 0)
    return dict(density_first=density_first, density_second=density_second, basis=basis, tile_list=tile_list, tile_count=tile_count, point_count=point_count, offsets=offsets, weights=weights, atom_of_point=atom_of_point)


def harmonics(offsets):
    first_axis = offsets[0]
    second_axis = offsets[1]
    third_axis = offsets[2]
    radius_sq = first_axis * first_axis + second_axis * second_axis + third_axis * third_axis
    return jnp.stack([jnp.ones_like(first_axis), first_axis, second_axis, third_axis,
                      first_axis * second_axis, second_axis * third_axis,
                      3.0 * third_axis * third_axis - radius_sq,
                      first_axis * third_axis,
                      first_axis * first_axis - second_axis * second_axis])


def storage_index(tiles, parts):
    per_part = NT // parts
    return ((tiles % parts) * per_part + tiles // parts).astype(jnp.int32)


def batch_density(stored_first, stored_second, values, tiles, live_tiles, live_points):
    inside = jnp.arange(TILE, dtype=jnp.int32)[None, :]
    rows = (storage_index(tiles, N_ROW)[:, None] * TILE + inside).reshape(-1)
    cols = (storage_index(tiles, N_COL)[:, None] * TILE + inside).reshape(-1)
    col_mask = jnp.repeat((jnp.arange(KT) < live_tiles).astype(jnp.bfloat16), TILE)
    masked = values * col_mask[None, :]
    point_mask = (jnp.arange(PTS) < live_points).astype(jnp.float32)
    results = []
    for stored in (stored_first, stored_second):
        block = stored[rows[:, None], cols[None, :]]
        product = jnp.dot(masked, block, preferred_element_type=jnp.float32)
        results.append(jnp.sum(product * masked.astype(jnp.float32), axis=1) * point_mask)
    return jnp.stack(results)


def reference(density_first, density_second, basis, tile_list, tile_count, point_count, offsets, weights, atom_of_point):
    def per_batch(inputs):
        values, tiles, live_tiles, live_points = inputs
        return batch_density(density_first, density_second, values, tiles, live_tiles, live_points)

    stacked = lax.map(per_batch, (basis, tile_list, tile_count, point_count))
    density = jnp.transpose(stacked, (1, 0, 2))
    harmonic = harmonics(offsets)
    moment_terms = density[:, None] * (weights[None, None] * harmonic[None])
    flat_terms = moment_terms.reshape(2 * 9, -1).T
    summed = jax.ops.segment_sum(flat_terms, atom_of_point.reshape(-1), num_segments=ATOMS)
    moments = summed.T.reshape(2, 9, ATOMS)
    return density, moments
```

```python
import jax
import jax.numpy as jnp
from jax import lax
from jax.experimental import pallas as pl
from jax.experimental.pallas import tpu as pltpu
from jax.sharding import Mesh
from jax.sharding import PartitionSpec as P

TILE = 128
KT = 7
NT = 96
PTS = 4096
ATOMS = 1024
N_ROW = 16
N_COL = 8
DEVICES = 128
SPAN = 12
ROW = ("row_0", "row_1")
COL = ("col_0", "col_1")
ROW_COL = ("row_0", "row_1", "col_0", "col_1")

SLOTS = 24
LINES = 32
PAIRS = KT * (KT + 1) // 2
WINDOW = 2 * PAIRS
FIRST = 32
REST = WINDOW - FIRST
FRONT = 1152
BACK = 1536
BLOCK = 512
STEPS = PTS // BLOCK
ROUNDER = 12582912.0


def pair_start(last):
    return last * (last + 1) // 2


def spread_body(place, own_start, first, second, out, tiles, lines, sems):
    my_row = place[0]
    my_col = place[1]
    lead = lax.rem(my_col - my_row + 16, 8)
    base = (my_row - my_col + lead) // 8
    copies = []
    for half in range(2):
        for step in range(6):
            for which, stored in enumerate((first, second)):
                index = which * 12 + half * 6 + step
                column = jnp.clip(2 * step + base - half, 0, 11)
                copy = pltpu.make_async_copy(
                    stored.at[pl.ds(step * TILE, TILE), pl.ds(pl.multiple_of(column * TILE, TILE), TILE)],
                    tiles.at[index],
                    sems.at[index],
                )
                copy.start()
                copies.append((copy, index, half, step))
    largest = jnp.zeros((8, TILE), jnp.float32)
    for copy, index, half, step in copies:
        copy.wait()
        values = tiles[index].astype(jnp.float32)
        column = 2 * step + base - half
        shift = lead - 8 * half
        used = (column >= 0) & (column < 12) & (shift <= 6) & (shift >= -6)
        peak = jnp.max(jnp.abs(values).reshape(16, 8, TILE), axis=0)
        largest = jnp.maximum(largest, jnp.where(used, peak, 0.0))
        if half:
            values = values.T
        lines[pl.ds(index, TILE, stride=SLOTS), :] = values
    peak = jnp.max(largest)
    line = lax.broadcasted_iota(jnp.int32, (8, TILE), 0)
    extra = jnp.where(
        line == 0,
        own_start[0].astype(jnp.float32),
        jnp.where(line == 1, own_start[1].astype(jnp.float32), peak),
    )

    def pack(dest, carry):
        at = pl.multiple_of(dest * SLOTS, 8)
        low = lines[pl.ds(at, 16), :]
        high = lines[pl.ds(at + 16, 8), :]
        to = pl.multiple_of(dest * LINES, 16)
        out[pl.ds(to, 16), :] = low.astype(jnp.bfloat16)
        out[pl.ds(to + 16, 16), :] = jnp.concatenate([high, extra], axis=0).astype(jnp.bfloat16)
        return carry

    lax.fori_loop(0, DEVICES, pack, 0, unroll=4)


def spread(place, own_start, first, second):
    return pl.pallas_call(
        spread_body,
        out_shape=jax.ShapeDtypeStruct((DEVICES * LINES, TILE), jnp.bfloat16),
        in_specs=[
            pl.BlockSpec(memory_space=pltpu.SMEM),
            pl.BlockSpec(memory_space=pltpu.SMEM),
            pl.BlockSpec(memory_space=pl.ANY),
            pl.BlockSpec(memory_space=pl.ANY),
        ],
        out_specs=pl.BlockSpec(memory_space=pltpu.VMEM),
        scratch_shapes=[
            pltpu.VMEM((SLOTS, TILE, TILE), jnp.bfloat16),
            pltpu.VMEM((DEVICES * SLOTS, TILE), jnp.float32),
            pltpu.SemaphoreType.DMA((SLOTS,)),
        ],
        name="spread_rows",
    )(place, own_start, first, second)


def window_body(arrived, out_first, out_rest, unit_out, lines, coded, start_lines, starts, sem):
    def widen(source, top):
        at = pl.multiple_of(source * LINES, 16)
        to = pl.multiple_of(FRONT + source * SLOTS, 8)
        low = arrived[pl.ds(at, 16), :].astype(jnp.float32)
        high = arrived[pl.ds(at + 16, 16), :].astype(jnp.float32)
        lines[pl.ds(to, 16), :] = low
        lines[pl.ds(to + 16, 8), :] = high[0:8]
        extra = high[8:16]
        peak, own = top
        lane = lax.broadcasted_iota(jnp.int32, (8, TILE), 1)
        own = jnp.where(lane == source, extra, own)
        return jnp.maximum(peak, extra), own

    zero = jnp.zeros((8, TILE), jnp.float32)
    tops, own = lax.fori_loop(0, DEVICES, widen, (zero, zero), unroll=4)
    start_lines[...] = own.astype(jnp.int32)
    copy = pltpu.make_async_copy(start_lines, starts, sem)
    copy.start()
    peak = jnp.broadcast_to(tops[2:3, :], (8, TILE))
    scale = jnp.full((8, TILE), 2.0**21, jnp.float32)
    unit = jnp.full((8, TILE), 2.0**-21, jnp.float32)
    for step in range(1, 64):
        small = peak < 2.0 ** (-7 - step)
        scale = jnp.where(small, 2.0 ** (21 + step), scale)
        unit = jnp.where(small, 2.0 ** (-21 - step), unit)
    unit_out[...] = unit

    order = lax.broadcasted_iota(jnp.int32, (8, TILE), 0)

    def line_of(row, col, which, half, step):
        return FRONT + (row * N_COL + col) * SLOTS + which * 12 + half * 6 + step

    def eight(start):
        return lines[pl.ds(start, 8, stride=(N_COL + 1) * SLOTS), :]

    for apart in range(KT):
        for group in range(NT // 8):
            words = []
            for which in range(2):
                odd = group % 2
                step = group // 2
                if odd or apart == 0:
                    total = eight(line_of(8 * odd - apart, 0, which, 0, step))
                else:
                    total = eight(line_of(-apart, 0, which, 0, step))
                    if step > 0:
                        before = eight(line_of(16 - apart, 0, which, 0, step - 1))
                        total = jnp.where(order < apart, before, total)
                if apart > 0:
                    after = eight(line_of(8 * odd, -apart, which, 1, step))
                    wrapped = eight(line_of(8 * odd, 8 - apart, which, 1, step))
                    total = total + jnp.where(order < apart, wrapped, after)
                total = total * scale
                words.append(((total + ROUNDER) - ROUNDER).astype(jnp.int32))
            word = (words[0] << 16) | (words[1] & 0xFFFF)
            coded[pl.ds(group * 64 + apart, 8, stride=8), :] = word

    copy.wait()

    def fill(dest, carry):
        for batch in range(2):
            begin = starts[batch, dest]
            for last in range(KT):
                words = coded[pl.ds(pl.multiple_of((begin + last) * 8, 8), 8), :]
                low = batch * PAIRS + pair_start(last)
                high = low + last + 1
                if low < FIRST:
                    cut = min(high, FIRST)
                    out_first[dest, low:cut, :] = words[0 : cut - low]
                if high > FIRST:
                    cut = max(low, FIRST)
                    out_rest[dest, cut - FIRST : high - FIRST, :] = words[cut - low : last + 1]
        return carry

    lax.fori_loop(0, DEVICES, fill, 0, unroll=2)


def windows(arrived):
    return pl.pallas_call(
        window_body,
        out_shape=(
            jax.ShapeDtypeStruct((DEVICES, FIRST, TILE), jnp.int32),
            jax.ShapeDtypeStruct((DEVICES, REST, TILE), jnp.int32),
            jax.ShapeDtypeStruct((8, TILE), jnp.float32),
        ),
        in_specs=[pl.BlockSpec(memory_space=pltpu.VMEM)],
        out_specs=tuple(pl.BlockSpec(memory_space=pltpu.VMEM) for _ in range(3)),
        scratch_shapes=[
            pltpu.VMEM((FRONT + DEVICES * SLOTS + BACK, TILE), jnp.float32),
            pltpu.VMEM((NT * 8, TILE), jnp.int32),
            pltpu.VMEM((8, TILE), jnp.int32),
            pltpu.SMEM((8, TILE), jnp.int32),
            pltpu.SemaphoreType.DMA,
        ],
        name="pick_windows",
    )(arrived)


def unit_at(batch, low, high):
    line = batch * PAIRS + pair_start(high) + (high - low)
    if line < FIRST:
        return 0, line
    return 1, line - FIRST


def batch_body(batch, table, *refs):
    data = refs[:2] if batch else (refs[0], None)
    refs = refs[2:] if batch else refs[1:]
    unit, offsets, weights, atoms = refs[:4]
    basis = refs[4 : 4 + KT]
    density, payload = refs[4 + KT : 6 + KT]
    high_part, low_part = refs[6 + KT :]
    step = pl.program_id(0)
    live_points = table[14]
    base_atom = table[15]

    @pl.when(step == 0)
    def _():
        zero = jnp.zeros((TILE, TILE), jnp.bfloat16)
        for last in range(KT):
            for first in range(last + 1):
                which, line = unit_at(batch, first, last)
                length = REST if which else FIRST
                words = data[which][pl.ds(line, TILE, stride=length), :]
                keep = table[7 + first] * table[7 + last]
                for matrix in range(2):
                    value = words >> 16 if matrix == 0 else (words << 16) >> 16
                    value = (value * keep).astype(jnp.float32)
                    top = value.astype(jnp.bfloat16)
                    rows = slice(first * TILE, (first + 1) * TILE)
                    at = (last + matrix * KT if last < KT - 1 else 12 + matrix) * TILE
                    if last < KT - 1:
                        at = (last + matrix * (KT - 1)) * TILE
                    high_part[rows, at : at + TILE] = top
                    if first < last:
                        bottom = (value - top.astype(jnp.float32)).astype(jnp.bfloat16)
                        low_part[rows, at : at + TILE] = bottom
        for matrix in range(2):
            for pair in range(3):
                at = (2 * pair + matrix * (KT - 1)) * TILE
                rows = slice((2 * pair + 1) * TILE, (2 * pair + 2) * TILE)
                high_part[rows, at : at + TILE] = zero
                rows = slice(2 * pair * TILE, (2 * pair + 1) * TILE)
                low_part[rows, at : at + TILE] = zero

    start = pl.multiple_of(step * BLOCK, BLOCK)

    @pl.when(start >= live_points)
    def _():
        density[:, pl.ds(start, BLOCK)] = jnp.zeros((2, BLOCK), jnp.float32)

    @pl.when(start < live_points)
    def _():
        columns = [ref[...] for ref in basis]
        values = jnp.concatenate(columns, axis=1)
        sums = [None, None]

        def product(at, tiles, top_rows, low_rows):
            ahead = jnp.dot(
                values[:, :top_rows], high_part[:top_rows, at : at + tiles * TILE],
                preferred_element_type=jnp.float32,
            )
            return ahead + jnp.dot(
                values[:, :low_rows], low_part[:low_rows, at : at + tiles * TILE],
                preferred_element_type=jnp.float32,
            )

        def add(matrix, part):
            sums[matrix] = part if sums[matrix] is None else sums[matrix] + part

        for pair in range(3):
            for matrix in range(2):
                at = (2 * pair + matrix * (KT - 1)) * TILE
                got = product(at, 2, (2 * pair + 2) * TILE, (2 * pair + 1) * TILE)
                add(matrix, got[:, :TILE] * columns[2 * pair].astype(jnp.float32))
                add(matrix, got[:, TILE:] * columns[2 * pair + 1].astype(jnp.float32))
        got = product(12 * TILE, 2, KT * TILE, (KT - 1) * TILE)
        last = columns[KT - 1].astype(jnp.float32)
        add(0, got[:, :TILE] * last)
        add(1, got[:, TILE:] * last)
        point = start + lax.broadcasted_iota(jnp.int32, (1, BLOCK), 1)
        scale = jnp.where(point < live_points, unit[0:1, 0:1], 0.0)
        for matrix in range(2):
            line = jnp.concatenate(
                [
                    jnp.sum(sums[matrix][cut : cut + TILE].T, axis=0, keepdims=True)
                    for cut in range(0, BLOCK, TILE)
                ],
                axis=1,
            )
            density[matrix : matrix + 1, pl.ds(start, BLOCK)] = line * scale

    @pl.when(step == STEPS - 1)
    def _():
        x = offsets[0, batch : batch + 1, :]
        y = offsets[1, batch : batch + 1, :]
        z = offsets[2, batch : batch + 1, :]
        weight = weights[batch : batch + 1, :]
        near = lax.rem(atoms[batch : batch + 1, :] - base_atom + 2 * ATOMS, ATOMS)
        squared = x * x + y * y + z * z
        shapes = [
            jnp.ones_like(x), x, y, z, x * y, y * z,
            3.0 * z * z - squared, x * z, x * x - y * y,
        ]
        shapes = jnp.concatenate([weight * shape for shape in shapes], axis=0)
        lane = lax.broadcasted_iota(jnp.int32, (9, TILE), 1)
        degree = lax.broadcasted_iota(jnp.int32, (9, TILE), 0)
        lane = lane - degree * SPAN
        for matrix in range(2):
            terms = density[matrix : matrix + 1, :] * shapes
            total = jnp.zeros((9, TILE), jnp.float32)
            for atom in range(8):
                picked = jnp.sum(jnp.where(near == atom, terms, 0.0), axis=1, keepdims=True)
                total = total + jnp.where(lane == atom + 4 * batch, picked, 0.0)
            payload[matrix : matrix + 1, :] = jnp.sum(total, axis=0, keepdims=True)


def batch_call(batch, table, data, unit, offsets, weights, atoms, basis):
    def whole(array):
        return pl.BlockSpec(array.shape, lambda i, t, n=array.ndim: (0,) * n)

    def column(place):
        def index(i, t):
            top = jnp.maximum(t[14] - 1, 0) // BLOCK
            return (batch * STEPS + jnp.minimum(i, top), t[place])

        return pl.BlockSpec((BLOCK, TILE), index)

    arrays = [*data, unit, offsets, weights, atoms]
    spec = pltpu.PrefetchScalarGridSpec(
        num_scalar_prefetch=1,
        grid=(STEPS,),
        in_specs=[whole(array) for array in arrays] + [column(place) for place in range(KT)],
        out_specs=(
            pl.BlockSpec((2, PTS), lambda i, t: (0, 0)),
            pl.BlockSpec((2, TILE), lambda i, t: (0, 0)),
        ),
        scratch_shapes=[
            pltpu.VMEM((KT * TILE, 14 * TILE), jnp.bfloat16),
            pltpu.VMEM((KT * TILE, 14 * TILE), jnp.bfloat16),
        ],
    )

    def body(*refs):
        batch_body(batch, *refs)

    return pl.pallas_call(
        body,
        grid_spec=spec,
        out_shape=(
            jax.ShapeDtypeStruct((2, PTS), jnp.float32),
            jax.ShapeDtypeStruct((2, TILE), jnp.float32),
        ),
        compiler_params=pltpu.CompilerParams(vmem_limit_bytes=60 * 1024 * 1024),
        cost_estimate=pl.CostEstimate(
            flops=26_000_000_000, bytes_accessed=10_000_000, transcendentals=0
        ),
        name=f"batch_density_{batch}",
    )(table, *arrays, *([basis] * KT))


def moment_body(arrived, out):
    lane = lax.broadcasted_iota(jnp.int32, (8, TILE), 1)
    for matrix in range(2):
        totals = [jnp.zeros((8, TILE), jnp.float32) for _ in range(9)]
        for place in range(16):
            part = arrived[pl.ds(2 * place + matrix, 8, stride=32), :]
            for degree in range(9):
                moved = pltpu.roll(part, (8 * place - SPAN * degree) % TILE, 1)
                if place < 15:
                    mine = (lane >= 8 * place) & (lane < 8 * place + SPAN)
                    totals[degree] = totals[degree] + jnp.where(mine, moved, 0.0)
                else:
                    inside = jnp.where(lane >= 8 * place, moved, 0.0)
                    after = pltpu.roll(jnp.where(lane < SPAN - 8, moved, 0.0), 1, 0)
                    totals[degree] = totals[degree] + inside + after
        for degree in range(9):
            for block in range(8):
                out[matrix, degree : degree + 1, block * TILE : (block + 1) * TILE] = totals[degree][
                    block : block + 1, :
                ]


def moment_table(arrived):
    return pl.pallas_call(
        moment_body,
        out_shape=jax.ShapeDtypeStruct((2, 9, ATOMS), jnp.float32),
        in_specs=[pl.BlockSpec(memory_space=pltpu.VMEM)],
        out_specs=pl.BlockSpec(memory_space=pltpu.VMEM),
        name="moment_table",
    )(arrived)


def exchange(value):
    return lax.all_to_all(value, ROW_COL, 0, 0, tiled=True)


def local(
    density_first,
    density_second,
    basis,
    tile_list,
    tile_count,
    point_count,
    offsets,
    weights,
    atom_of_point,
):
    my_row = lax.axis_index(ROW)
    my_col = lax.axis_index(COL)
    device = my_row * N_COL + my_col
    own_start = jnp.min(tile_list, axis=1)
    place = jnp.stack([my_row, my_col]).astype(jnp.int32)
    rows = spread(place, own_start, density_first, density_second)
    rows = exchange(rows.reshape(DEVICES, LINES, TILE)).reshape(DEVICES * LINES, TILE)
    first, rest, unit = windows(rows)
    first = exchange(first).reshape(DEVICES * FIRST, TILE)
    rest = exchange(rest).reshape(DEVICES * REST, TILE)

    relative = tile_list - own_start[:, None]
    hit = relative[:, None, :] == jnp.arange(KT, dtype=jnp.int32)[None, :, None]
    column = jnp.sum(jnp.where(hit, jnp.arange(KT, dtype=jnp.int32)[None, None, :], 0), axis=2)
    live = (column < tile_count[:, None]).astype(jnp.int32)
    first_atom = (2 * device + jnp.arange(2, dtype=jnp.int32)) * 4 % ATOMS
    table = jnp.concatenate(
        [column, live, point_count[:, None], first_atom[:, None].astype(jnp.int32)], axis=1
    ).astype(jnp.int32)
    flat = basis.reshape(-1, KT * TILE)
    side = (unit, offsets, weights, atom_of_point)
    density_0, payload_0 = batch_call(0, table[0], (first,), *side, flat)
    density_1, payload_1 = batch_call(1, table[1], (first, rest), *side, flat)
    density = jnp.stack([density_0, density_1], axis=1)
    payload = payload_0 + payload_1
    spread_out = jnp.broadcast_to(payload[None], (DEVICES, 2, TILE))
    moments = moment_table(exchange(spread_out).reshape(DEVICES * 2, TILE))
    return density, moments


def solution(mesh):
    torus = Mesh(mesh.devices.reshape(4, 4, 4, 2), ("row_0", "row_1", "col_0", "col_1"))
    in_specs = (
        P(ROW, COL),
        P(ROW, COL),
        P(ROW_COL, None, None),
        P(ROW_COL, None),
        P(ROW_COL),
        P(ROW_COL),
        P(None, ROW_COL, None),
        P(ROW_COL, None),
        P(ROW_COL, None),
    )
    out_specs = (P(None, ROW_COL, None), P())
    return jax.shard_map(local, mesh=torus, in_specs=in_specs, out_specs=out_specs, check_vma=False)
```

```python
import jax
import jax.numpy as jnp
from jax import lax
from jax.experimental import pallas as pl
from jax.experimental.pallas import tpu as pltpu
from jax.sharding import Mesh
from jax.sharding import PartitionSpec as P

TILE = 128
KT = 7
NT = 96
PTS = 4096
ATOMS = 1024
N_ROW = 16
N_COL = 8
DEVICES = 128
SPAN = 12
ROW = ("row_0", "row_1")
COL = ("col_0", "col_1")
ROW_COL = ("row_0", "row_1", "col_0", "col_1")

SLOTS = 24
LINES = 32
PAIRS = KT * (KT + 1) // 2
WINDOW = 2 * PAIRS
FIRST = 32
REST = WINDOW - FIRST
FRONT = 1152
BACK = 1536
BLOCK = 512
STEPS = PTS // BLOCK
ROUNDER = 12582912.0


def pair_start(last):
    return last * (last + 1) // 2


def spread_body(tile_list, first, second, out, tiles, lines, sems):
    my_row = lax.axis_index(ROW)
    my_col = lax.axis_index(COL)
    own_start = []
    for batch in range(2):
        least = tile_list[batch, 0]
        for place in range(1, KT):
            least = jnp.minimum(least, tile_list[batch, place])
        own_start.append(least)
    lead = lax.rem(my_col - my_row + 16, 8)
    base = (my_row - my_col + lead) // 8
    copies = []
    for half in range(2):
        for step in range(6):
            for which, stored in enumerate((first, second)):
                index = which * 12 + half * 6 + step
                column = jnp.clip(2 * step + base - half, 0, 11)
                copy = pltpu.make_async_copy(
                    stored.at[pl.ds(step * TILE, TILE), pl.ds(pl.multiple_of(column * TILE, TILE), TILE)],
                    tiles.at[index],
                    sems.at[index],
                )
                copy.start()
                copies.append((copy, index, half, step))
    largest = jnp.zeros((8, TILE), jnp.float32)
    for copy, index, half, step in copies:
        copy.wait()
        values = tiles[index].astype(jnp.float32)
        column = 2 * step + base - half
        shift = lead - 8 * half
        used = (column >= 0) & (column < 12) & (shift <= 6) & (shift >= -6)
        peak = jnp.max(jnp.abs(values).reshape(16, 8, TILE), axis=0)
        largest = jnp.maximum(largest, jnp.where(used, peak, 0.0))
        if half:
            values = values.T
        lines[pl.ds(index, TILE, stride=SLOTS), :] = values
    peak = jnp.max(largest)
    line = lax.broadcasted_iota(jnp.int32, (8, TILE), 0)
    extra = jnp.where(
        line == 0,
        own_start[0].astype(jnp.float32),
        jnp.where(line == 1, own_start[1].astype(jnp.float32), peak),
    )

    def pack(dest, carry):
        at = pl.multiple_of(dest * SLOTS, 8)
        low = lines[pl.ds(at, 16), :]
        high = lines[pl.ds(at + 16, 8), :]
        to = pl.multiple_of(dest * LINES, 16)
        out[pl.ds(to, 16), :] = low.astype(jnp.bfloat16)
        out[pl.ds(to + 16, 16), :] = jnp.concatenate([high, extra], axis=0).astype(jnp.bfloat16)
        return carry

    lax.fori_loop(0, DEVICES, pack, 0, unroll=4)


def spread(tile_list, first, second):
    return pl.pallas_call(
        spread_body,
        out_shape=jax.ShapeDtypeStruct((DEVICES * LINES, TILE), jnp.bfloat16),
        in_specs=[
            pl.BlockSpec(memory_space=pltpu.SMEM),
            pl.BlockSpec(memory_space=pl.ANY),
            pl.BlockSpec(memory_space=pl.ANY),
        ],
        out_specs=pl.BlockSpec(memory_space=pltpu.VMEM),
        scratch_shapes=[
            pltpu.VMEM((SLOTS, TILE, TILE), jnp.bfloat16),
            pltpu.VMEM((DEVICES * SLOTS, TILE), jnp.float32),
            pltpu.SemaphoreType.DMA((SLOTS,)),
        ],
        name="spread_rows",
    )(tile_list, first, second)


def window_body(arrived, out_first, out_rest, unit_out, lines, coded, start_lines, starts, sem):
    def widen(source, top):
        at = pl.multiple_of(source * LINES, 16)
        to = pl.multiple_of(FRONT + source * SLOTS, 8)
        low = arrived[pl.ds(at, 16), :].astype(jnp.float32)
        high = arrived[pl.ds(at + 16, 16), :].astype(jnp.float32)
        lines[pl.ds(to, 16), :] = low
        lines[pl.ds(to + 16, 8), :] = high[0:8]
        extra = high[8:16]
        peak, own = top
        lane = lax.broadcasted_iota(jnp.int32, (8, TILE), 1)
        own = jnp.where(lane == source, extra, own)
        return jnp.maximum(peak, extra), own

    zero = jnp.zeros((8, TILE), jnp.float32)
    tops, own = lax.fori_loop(0, DEVICES, widen, (zero, zero), unroll=4)
    start_lines[...] = own.astype(jnp.int32)
    copy = pltpu.make_async_copy(start_lines, starts, sem)
    copy.start()
    peak = jnp.broadcast_to(tops[2:3, :], (8, TILE))
    scale = jnp.full((8, TILE), 2.0**21, jnp.float32)
    unit = jnp.full((8, TILE), 2.0**-21, jnp.float32)
    for step in range(1, 64):
        small = peak < 2.0 ** (-7 - step)
        scale = jnp.where(small, 2.0 ** (21 + step), scale)
        unit = jnp.where(small, 2.0 ** (-21 - step), unit)
    unit_out[...] = unit

    order = lax.broadcasted_iota(jnp.int32, (8, TILE), 0)

    def line_of(row, col, which, half, step):
        return FRONT + (row * N_COL + col) * SLOTS + which * 12 + half * 6 + step

    def eight(start):
        return lines[pl.ds(start, 8, stride=(N_COL + 1) * SLOTS), :]

    for apart in range(KT):
        for group in range(NT // 8):
            words = []
            for which in range(2):
                odd = group % 2
                step = group // 2
                if odd or apart == 0:
                    total = eight(line_of(8 * odd - apart, 0, which, 0, step))
                else:
                    total = eight(line_of(-apart, 0, which, 0, step))
                    if step > 0:
                        before = eight(line_of(16 - apart, 0, which, 0, step - 1))
                        total = jnp.where(order < apart, before, total)
                if apart > 0:
                    after = eight(line_of(8 * odd, -apart, which, 1, step))
                    wrapped = eight(line_of(8 * odd, 8 - apart, which, 1, step))
                    total = total + jnp.where(order < apart, wrapped, after)
                total = total * scale
                words.append(((total + ROUNDER) - ROUNDER).astype(jnp.int32))
            word = (words[0] << 16) | (words[1] & 0xFFFF)
            coded[pl.ds(group * 64 + apart, 8, stride=8), :] = word

    copy.wait()

    def fill(dest, carry):
        for batch in range(2):
            begin = starts[batch, dest]
            for last in range(KT):
                words = coded[pl.ds(pl.multiple_of((begin + last) * 8, 8), 8), :]
                low = batch * PAIRS + pair_start(last)
                high = low + last + 1
                if low < FIRST:
                    cut = min(high, FIRST)
                    out_first[dest, low:cut, :] = words[0 : cut - low]
                if high > FIRST:
                    cut = max(low, FIRST)
                    out_rest[dest, cut - FIRST : high - FIRST, :] = words[cut - low : last + 1]
        return carry

    lax.fori_loop(0, DEVICES, fill, 0, unroll=2)


def windows(arrived):
    return pl.pallas_call(
        window_body,
        out_shape=(
            jax.ShapeDtypeStruct((DEVICES, FIRST, TILE), jnp.int32),
            jax.ShapeDtypeStruct((DEVICES, REST, TILE), jnp.int32),
            jax.ShapeDtypeStruct((8, TILE), jnp.float32),
        ),
        in_specs=[pl.BlockSpec(memory_space=pltpu.VMEM)],
        out_specs=tuple(pl.BlockSpec(memory_space=pltpu.VMEM) for _ in range(3)),
        scratch_shapes=[
            pltpu.VMEM((FRONT + DEVICES * SLOTS + BACK, TILE), jnp.float32),
            pltpu.VMEM((NT * 8, TILE), jnp.int32),
            pltpu.VMEM((8, TILE), jnp.int32),
            pltpu.SMEM((8, TILE), jnp.int32),
            pltpu.SemaphoreType.DMA,
        ],
        name="pick_windows",
    )(arrived)


def table_body(tile_list, tile_count, point_count, table):
    device = lax.axis_index(ROW) * N_COL + lax.axis_index(COL)
    for batch in range(2):
        start = tile_list[batch, 0]
        for place in range(1, KT):
            start = jnp.minimum(start, tile_list[batch, place])
        for place in range(KT):
            rank = tile_list[batch, place] - start
            table[batch * 16 + rank] = place
            table[batch * 16 + KT + rank] = (place < tile_count[batch]).astype(jnp.int32)
        table[batch * 16 + 14] = point_count[batch]
        table[batch * 16 + 15] = lax.rem((2 * device + batch) * 4, ATOMS)


def batch_tables(tile_list, tile_count, point_count):
    return pl.pallas_call(
        table_body,
        out_shape=jax.ShapeDtypeStruct((32,), jnp.int32),
        in_specs=[pl.BlockSpec(memory_space=pltpu.SMEM) for _ in range(3)],
        out_specs=pl.BlockSpec(memory_space=pltpu.SMEM),
        name="batch_tables",
    )(tile_list, tile_count, point_count)


def unit_at(batch, low, high):
    line = batch * PAIRS + pair_start(high) + (high - low)
    if line < FIRST:
        return 0, line
    return 1, line - FIRST


def first_blocks(batch):
    begin = batch * PAIRS // 8
    return range(begin, min(-(-(batch + 1) * PAIRS // 8), FIRST // 8))


def batch_body(batch, table, *refs):
    first_count = len(first_blocks(batch))
    first_rows = refs[:first_count]
    refs = refs[first_count:]

    def from_first(line):
        rows = first_rows[line // 8 - first_blocks(batch)[0]].reshape(DEVICES * 8, TILE)
        return rows[pl.ds(line % 8, TILE, stride=8), :]

    if batch:
        rest_rows = refs[0]
        before = refs[1]
        earlier = refs[2]
        refs = refs[3:]

        def from_rest(line):
            return rest_rows[pl.ds(line, TILE, stride=REST), :]

        data = (from_first, from_rest)
    else:
        data = (from_first, None)
    unit, offsets, weights, atoms = refs[:4]
    basis = refs[4 : 4 + KT]
    density, payload = refs[4 + KT : 6 + KT]
    high_part, low_part = refs[6 + KT :]
    step = pl.program_id(0)
    live_points = table[batch * 16 + 14]
    base_atom = table[batch * 16 + 15]

    @pl.when(step == 0)
    def _():
        for last in range(KT):
            for first in range(last + 1):
                which, line = unit_at(batch, first, last)
                words = data[which](line)
                keep = table[batch * 16 + KT + first] * table[batch * 16 + KT + last]
                rows = slice(first * TILE, (first + 1) * TILE)
                for matrix in range(2):
                    value = words >> 16 if matrix == 0 else (words << 16) >> 16
                    value = (value * keep).astype(jnp.float32)
                    top = value.astype(jnp.bfloat16)
                    at = (2 * last + matrix) * TILE
                    high_part[rows, at : at + TILE] = top
                    if first < last:
                        bottom = (value - top.astype(jnp.float32)).astype(jnp.bfloat16)
                        low_part[rows, at : at + TILE] = bottom

    start = pl.multiple_of(step * BLOCK, BLOCK)

    def put(start, lines):
        if batch:
            at = pl.ds(start, BLOCK)
            for matrix in range(2):
                both = [earlier[matrix : matrix + 1, at], lines[matrix : matrix + 1]]
                density[matrix, :, at] = jnp.concatenate(both, axis=0)
        else:
            density[:, pl.ds(start, BLOCK)] = lines

    @pl.when(start >= live_points)
    def _():
        put(start, jnp.zeros((2, BLOCK), jnp.float32))

    @pl.when(start < live_points)
    def _():
        columns = [ref[...] for ref in basis]
        values = jnp.concatenate(columns, axis=1)
        sums = [None, None]
        for last in range(KT):
            cols = slice(2 * last * TILE, (2 * last + 2) * TILE)
            rows = (last + 1) * TILE
            got = jnp.dot(
                values[:, :rows], high_part[:rows, cols], preferred_element_type=jnp.float32
            )
            if last:
                rows = last * TILE
                got = got + jnp.dot(
                    values[:, :rows], low_part[:rows, cols], preferred_element_type=jnp.float32
                )
            column = columns[last].astype(jnp.float32)
            for matrix in range(2):
                part = got[:, matrix * TILE : (matrix + 1) * TILE] * column
                sums[matrix] = part if last == 0 else sums[matrix] + part
        point = start + lax.broadcasted_iota(jnp.int32, (1, BLOCK), 1)
        scale = jnp.where(point < live_points, unit[0:1, 0:1], 0.0)
        lines = []
        for matrix in range(2):
            pieces = [
                jnp.sum(sums[matrix][cut : cut + TILE].T, axis=0, keepdims=True)
                for cut in range(0, BLOCK, TILE)
            ]
            lines.append(jnp.concatenate(pieces, axis=1) * scale)
        put(start, jnp.concatenate(lines, axis=0))

    @pl.when(step == STEPS - 1)
    def _():
        x = offsets[0, batch : batch + 1, :]
        y = offsets[1, batch : batch + 1, :]
        z = offsets[2, batch : batch + 1, :]
        weight = weights[batch : batch + 1, :]
        near = lax.rem(atoms[batch : batch + 1, :] - base_atom + 2 * ATOMS, ATOMS)
        squared = x * x + y * y + z * z
        shapes = [
            jnp.ones_like(x), x, y, z, x * y, y * z,
            3.0 * z * z - squared, x * z, x * x - y * y,
        ]
        shapes = jnp.concatenate([weight * shape for shape in shapes], axis=0)
        lane = lax.broadcasted_iota(jnp.int32, (9, TILE), 1)
        degree = lax.broadcasted_iota(jnp.int32, (9, TILE), 0)
        lane = lane - degree * SPAN
        for matrix in range(2):
            if batch:
                terms = density[matrix, batch : batch + 1, :] * shapes
            else:
                terms = density[matrix : matrix + 1, :] * shapes
            total = jnp.zeros((9, TILE), jnp.float32)
            for atom in range(8):
                picked = jnp.sum(jnp.where(near == atom, terms, 0.0), axis=1, keepdims=True)
                total = total + jnp.where(lane == atom + 4 * batch, picked, 0.0)
            line = jnp.sum(total, axis=0, keepdims=True)
            if batch:
                line = line + before[matrix : matrix + 1, :]
                payload[:, matrix : matrix + 1, :] = jnp.broadcast_to(line[None], (DEVICES, 1, TILE))
            else:
                payload[matrix : matrix + 1, :] = line


def batch_call(batch, table, data, unit, offsets, weights, atoms, basis):
    def whole(array):
        return pl.BlockSpec(array.shape, lambda i, t, n=array.ndim: (0,) * n)

    def column(place):
        def index(i, t):
            top = jnp.maximum(t[batch * 16 + 14] - 1, 0) // BLOCK
            return (batch * STEPS + jnp.minimum(i, top), t[batch * 16 + place])

        return pl.BlockSpec((BLOCK, TILE), index)

    blocks = first_blocks(batch)
    rest = [*data[1:], unit, offsets, weights, atoms]
    arrays = [data[0]] * len(blocks) + rest
    specs = [
        pl.BlockSpec((DEVICES, 8, TILE), lambda i, t, block=block: (0, block, 0)) for block in blocks
    ]
    specs += [whole(array) for array in rest]
    payload = (DEVICES, 2, TILE) if batch else (2, TILE)
    density = (2, 2, PTS) if batch else (2, PTS)
    spec = pltpu.PrefetchScalarGridSpec(
        num_scalar_prefetch=1,
        grid=(STEPS,),
        in_specs=specs + [column(place) for place in range(KT)],
        out_specs=(
            pl.BlockSpec(density, lambda i, t: (0,) * len(density)),
            pl.BlockSpec(payload, lambda i, t: (0,) * len(payload)),
        ),
        scratch_shapes=[
            pltpu.VMEM((KT * TILE, 2 * KT * TILE), jnp.bfloat16),
            pltpu.VMEM(((KT - 1) * TILE, 2 * KT * TILE), jnp.bfloat16),
        ],
    )

    def body(*refs):
        batch_body(batch, *refs)

    return pl.pallas_call(
        body,
        grid_spec=spec,
        out_shape=(
            jax.ShapeDtypeStruct(density, jnp.float32),
            jax.ShapeDtypeStruct(payload, jnp.float32),
        ),
        compiler_params=pltpu.CompilerParams(vmem_limit_bytes=60 * 1024 * 1024),
        cost_estimate=pl.CostEstimate(
            flops=26_000_000_000, bytes_accessed=10_000_000, transcendentals=0
        ),
        name=f"batch_density_{batch}",
    )(table, *arrays, *([basis] * KT))


def moment_body(arrived, out):
    lane = lax.broadcasted_iota(jnp.int32, (8, TILE), 1)
    for matrix in range(2):
        totals = [jnp.zeros((8, TILE), jnp.float32) for _ in range(9)]
        for place in range(16):
            part = arrived[pl.ds(2 * place + matrix, 8, stride=32), :]
            for degree in range(9):
                moved = pltpu.roll(part, (8 * place - SPAN * degree) % TILE, 1)
                if place < 15:
                    mine = (lane >= 8 * place) & (lane < 8 * place + SPAN)
                    totals[degree] = totals[degree] + jnp.where(mine, moved, 0.0)
                else:
                    inside = jnp.where(lane >= 8 * place, moved, 0.0)
                    after = pltpu.roll(jnp.where(lane < SPAN - 8, moved, 0.0), 1, 0)
                    totals[degree] = totals[degree] + inside + after
        for degree in range(9):
            for block in range(8):
                out[degree, matrix : matrix + 1, block * TILE : (block + 1) * TILE] = totals[degree][
                    block : block + 1, :
                ]


def moment_table(arrived):
    return pl.pallas_call(
        moment_body,
        out_shape=jax.ShapeDtypeStruct((9, 2, ATOMS), jnp.float32),
        in_specs=[pl.BlockSpec(memory_space=pltpu.VMEM)],
        out_specs=pl.BlockSpec(memory_space=pltpu.VMEM),
        name="moment_table",
    )(arrived)


def exchange(value):
    return lax.all_to_all(value, ROW_COL, 0, 0, tiled=True)


def local(
    density_first,
    density_second,
    basis,
    tile_list,
    tile_count,
    point_count,
    offsets,
    weights,
    atom_of_point,
):
    rows = spread(tile_list, density_first, density_second)
    rows = exchange(rows.reshape(DEVICES, LINES, TILE)).reshape(DEVICES * LINES, TILE)
    first, rest, unit = windows(rows)
    with jax.named_scope("send_first"):
        first = exchange(first)
    with jax.named_scope("send_rest"):
        rest = exchange(rest)

    table = batch_tables(tile_list, tile_count, point_count)
    flat = basis.reshape(-1, KT * TILE)
    side = (unit, offsets, weights, atom_of_point)
    density_0, payload_0 = batch_call(
        0, table, (first,), *side, flat
    )
    rest = rest.reshape(DEVICES * REST, TILE)
    density, payload = batch_call(1, table, (first, rest, payload_0, density_0), *side, flat)
    moments = moment_table(exchange(payload).reshape(DEVICES * 2, TILE)).swapaxes(0, 1)
    return density, moments


def solution(mesh):
    torus = Mesh(mesh.devices.reshape(4, 4, 4, 2), ("row_0", "row_1", "col_0", "col_1"))
    in_specs = (
        P(ROW, COL),
        P(ROW, COL),
        P(ROW_COL, None, None),
        P(ROW_COL, None),
        P(ROW_COL),
        P(ROW_COL),
        P(None, ROW_COL, None),
        P(ROW_COL, None),
        P(ROW_COL, None),
    )
    out_specs = (P(None, ROW_COL, None), P())
    return jax.shard_map(local, mesh=torus, in_specs=in_specs, out_specs=out_specs, check_vma=False)
```

```python
import jax
import jax.numpy as jnp
from jax import lax
from jax.experimental import pallas as pl
from jax.experimental.pallas import tpu as pltpu
from jax.sharding import Mesh
from jax.sharding import PartitionSpec as P

TILE = 128
KT = 7
NT = 96
PTS = 4096
ATOMS = 1024
N_ROW = 16
N_COL = 8
DEVICES = 128
SPAN = 12
ROW = ("row_0", "row_1")
COL = ("col_0", "col_1")
ROW_COL = ("row_0", "row_1", "col_0", "col_1")

SLOTS = 24
LINES = 32
PAIRS = KT * (KT + 1) // 2
WINDOW = 2 * PAIRS
FIRST = 32
REST = WINDOW - FIRST
SLOT_LINES = 24
FRONT = 1152
BACK = 1536
BLOCK = 1024
STEPS = PTS // BLOCK
ROUNDER = 12582912.0


def pair_start(last):
    return last * (last + 1) // 2


def spread_body(tile_list, tile_count, point_count, first, second, out, tiles, lines, sems):
    my_row = lax.axis_index(ROW)
    my_col = lax.axis_index(COL)
    own_start = [least_tile(tile_list, batch) for batch in slot_order(tile_count, point_count)]
    lead = lax.rem(my_col - my_row + 16, 8)
    base = (my_row - my_col + lead) // 8
    copies = []
    for half in range(2):
        for step in range(6):
            for which, stored in enumerate((first, second)):
                index = which * 12 + half * 6 + step
                column = jnp.clip(2 * step + base - half, 0, 11)
                copy = pltpu.make_async_copy(
                    stored.at[pl.ds(step * TILE, TILE), pl.ds(pl.multiple_of(column * TILE, TILE), TILE)],
                    tiles.at[index],
                    sems.at[index],
                )
                copy.start()
                copies.append((copy, index, half, step))
    largest = jnp.zeros((8, TILE), jnp.float32)
    for copy, index, half, step in copies:
        copy.wait()
        values = tiles[index].astype(jnp.float32)
        column = 2 * step + base - half
        shift = lead - 8 * half
        used = (column >= 0) & (column < 12) & (shift <= 6) & (shift >= -6)
        peak = jnp.max(jnp.abs(values).reshape(16, 8, TILE), axis=0)
        largest = jnp.maximum(largest, jnp.where(used, peak, 0.0))
        if half:
            values = values.T
        lines[pl.ds(index, TILE, stride=SLOTS), :] = values
    peak = jnp.max(largest)
    line = lax.broadcasted_iota(jnp.int32, (8, TILE), 0)
    extra = jnp.where(
        line == 0,
        own_start[0].astype(jnp.float32),
        jnp.where(line == 1, own_start[1].astype(jnp.float32), peak),
    )

    def pack(dest, carry):
        at = pl.multiple_of(dest * SLOTS, 8)
        low = lines[pl.ds(at, 16), :]
        high = lines[pl.ds(at + 16, 8), :]
        to = pl.multiple_of(dest * LINES, 16)
        out[pl.ds(to, 16), :] = low.astype(jnp.bfloat16)
        out[pl.ds(to + 16, 16), :] = jnp.concatenate([high, extra], axis=0).astype(jnp.bfloat16)
        return carry

    lax.fori_loop(0, DEVICES, pack, 0, unroll=4)


def spread(tile_list, tile_count, point_count, first, second):
    return pl.pallas_call(
        spread_body,
        out_shape=jax.ShapeDtypeStruct((DEVICES * LINES, TILE), jnp.bfloat16),
        in_specs=[
            pl.BlockSpec(memory_space=pltpu.SMEM),
            pl.BlockSpec(memory_space=pltpu.SMEM),
            pl.BlockSpec(memory_space=pltpu.SMEM),
            pl.BlockSpec(memory_space=pl.ANY),
            pl.BlockSpec(memory_space=pl.ANY),
        ],
        out_specs=pl.BlockSpec(memory_space=pltpu.VMEM),
        scratch_shapes=[
            pltpu.VMEM((SLOTS, TILE, TILE), jnp.bfloat16),
            pltpu.VMEM((DEVICES * SLOTS, TILE), jnp.float32),
            pltpu.SemaphoreType.DMA((SLOTS,)),
        ],
        name="spread_rows",
    )(tile_list, tile_count, point_count, first, second)


def window_body(arrived, out_first, out_rest, unit_out, lines, coded, start_lines, starts, sem):
    def widen(source, top):
        at = pl.multiple_of(source * LINES, 16)
        to = pl.multiple_of(FRONT + source * SLOTS, 8)
        low = arrived[pl.ds(at, 16), :].astype(jnp.float32)
        high = arrived[pl.ds(at + 16, 16), :].astype(jnp.float32)
        lines[pl.ds(to, 16), :] = low
        lines[pl.ds(to + 16, 8), :] = high[0:8]
        extra = high[8:16]
        peak, own = top
        lane = lax.broadcasted_iota(jnp.int32, (8, TILE), 1)
        own = jnp.where(lane == source, extra, own)
        return jnp.maximum(peak, extra), own

    zero = jnp.zeros((8, TILE), jnp.float32)
    tops, own = lax.fori_loop(0, DEVICES, widen, (zero, zero), unroll=4)
    start_lines[...] = own.astype(jnp.int32)
    copy = pltpu.make_async_copy(start_lines, starts, sem)
    copy.start()
    peak = jnp.broadcast_to(tops[2:3, :], (8, TILE))
    scale = jnp.full((8, TILE), 2.0**21, jnp.float32)
    unit = jnp.full((8, TILE), 2.0**-21, jnp.float32)
    for step in range(1, 64):
        small = peak < 2.0 ** (-7 - step)
        scale = jnp.where(small, 2.0 ** (21 + step), scale)
        unit = jnp.where(small, 2.0 ** (-21 - step), unit)
    unit_out[...] = unit

    order = lax.broadcasted_iota(jnp.int32, (8, TILE), 0)

    def line_of(row, col, which, half, step):
        return FRONT + (row * N_COL + col) * SLOTS + which * 12 + half * 6 + step

    def eight(start):
        return lines[pl.ds(start, 8, stride=(N_COL + 1) * SLOTS), :]

    for apart in range(KT):
        for group in range(NT // 8):
            words = []
            for which in range(2):
                odd = group % 2
                step = group // 2
                if odd or apart == 0:
                    total = eight(line_of(8 * odd - apart, 0, which, 0, step))
                else:
                    total = eight(line_of(-apart, 0, which, 0, step))
                    if step > 0:
                        before = eight(line_of(16 - apart, 0, which, 0, step - 1))
                        total = jnp.where(order < apart, before, total)
                if apart > 0:
                    after = eight(line_of(8 * odd, -apart, which, 1, step))
                    wrapped = eight(line_of(8 * odd, 8 - apart, which, 1, step))
                    total = total + jnp.where(order < apart, wrapped, after)
                total = total * scale
                words.append(((total + ROUNDER) - ROUNDER).astype(jnp.int32))
            word = (words[0] << 16) | (words[1] & 0xFFFF)
            coded[pl.ds(group * 64 + apart, 8, stride=8), :] = word

    copy.wait()

    def fill(dest, carry):
        for batch in range(2):
            begin = starts[batch, dest]
            for last in range(KT):
                words = coded[pl.ds(pl.multiple_of((begin + last) * 8, 8), 8), :]
                low = batch * PAIRS + pair_start(last)
                high = low + last + 1
                if low < FIRST:
                    cut = min(high, FIRST)
                    out_first[dest, low:cut, :] = words[0 : cut - low]
                if high > FIRST:
                    cut = max(low, FIRST)
                    out_rest[dest, cut - FIRST : high - FIRST, :] = words[cut - low : last + 1]
        return carry

    lax.fori_loop(0, DEVICES, fill, 0, unroll=2)


def windows(arrived):
    return pl.pallas_call(
        window_body,
        out_shape=(
            jax.ShapeDtypeStruct((DEVICES, FIRST, TILE), jnp.int32),
            jax.ShapeDtypeStruct((DEVICES, REST, TILE), jnp.int32),
            jax.ShapeDtypeStruct((8, TILE), jnp.float32),
        ),
        in_specs=[pl.BlockSpec(memory_space=pltpu.VMEM)],
        out_specs=tuple(pl.BlockSpec(memory_space=pltpu.VMEM) for _ in range(3)),
        scratch_shapes=[
            pltpu.VMEM((FRONT + DEVICES * SLOTS + BACK, TILE), jnp.float32),
            pltpu.VMEM((NT * 8, TILE), jnp.int32),
            pltpu.VMEM((8, TILE), jnp.int32),
            pltpu.SMEM((8, TILE), jnp.int32),
            pltpu.SemaphoreType.DMA,
        ],
        name="pick_windows",
    )(arrived)


def slot_order(tile_count, point_count):
    work = []
    for batch in range(2):
        count = tile_count[batch]
        passes = jnp.where(count >= KT, 28, jnp.where(count == KT - 1, 21, 15))
        work.append(passes * point_count[batch])
    swap = (work[1] > work[0]).astype(jnp.int32)
    return swap, 1 - swap


def least_tile(tile_list, batch):
    least = tile_list[batch, 0]
    for place in range(1, KT):
        least = jnp.minimum(least, tile_list[batch, place])
    return least


COUNT = 7
POINTS = 8
ATOM = 9
BATCH = 10
LINE = 11
ENTRIES = 40


def table_body(tile_list, tile_count, point_count, table, column_of, order_of):
    device = lax.axis_index(ROW) * N_COL + lax.axis_index(COL)
    for slot, batch in enumerate(slot_order(tile_count, point_count)):
        base = slot * ENTRIES
        start = least_tile(tile_list, batch)
        count = jnp.minimum(tile_count[batch], KT)
        for place in range(KT):
            column_of[tile_list[batch, place] - start] = place
        live_end = 0
        dead_end = count
        for rank in range(KT):
            place = column_of[rank]
            live = (place < count).astype(jnp.int32)
            to = jnp.where(live == 1, live_end, dead_end)
            table[base + to] = place
            order_of[to] = rank
            live_end = live_end + live
            dead_end = dead_end + 1 - live
        table[base + COUNT] = count
        table[base + POINTS] = point_count[batch]
        table[base + ATOM] = lax.rem((2 * device + batch) * 4, ATOMS)
        table[base + BATCH] = batch
        for last in range(KT):
            high = order_of[last]
            for first in range(last + 1):
                low = order_of[first]
                line = slot * (PAIRS - SLOT_LINES) + high * (high + 1) // 2 + high - low
                line = jnp.where(last < count, line, SLOT_LINES)
                table[base + LINE + pair_start(last) + first] = (line // 8) * (DEVICES * 8) + line % 8


def batch_tables(tile_list, tile_count, point_count):
    return pl.pallas_call(
        table_body,
        out_shape=jax.ShapeDtypeStruct((2 * ENTRIES,), jnp.int32),
        in_specs=[pl.BlockSpec(memory_space=pltpu.SMEM) for _ in range(3)],
        out_specs=pl.BlockSpec(memory_space=pltpu.SMEM),
        scratch_shapes=[pltpu.SMEM((8,), jnp.int32), pltpu.SMEM((8,), jnp.int32)],
        name="batch_tables",
    )(tile_list, tile_count, point_count)


def batch_body(slot, *refs):
    table_in, first_rows = refs[:2]
    refs = refs[2:]
    if slot:
        rest_rows, before_in, earlier_in = refs[:3]
        refs = refs[3:]
        sources = [first_rows.at[:, pl.ds(FIRST - 8, 8), :]]
        sources += [rest_rows.at[:, pl.ds(8 * group, 8), :] for group in range(REST // 8)]
    else:
        sources = [first_rows.at[:, pl.ds(8 * group, 8), :] for group in range(FIRST // 8)]
    unit_in, offsets_in, weights_in, atoms_in, basis, density_out, payload_out = refs[:7]
    (
        table, high_part, low_part, rows, values_in, density, payload,
        unit, offsets, weights, atoms, before, earlier, sums_kept,
        table_sem, row_sems, value_sems, side_sems, out_sems,
    ) = refs[7:]
    base = slot * ENTRIES

    table_copy = pltpu.make_async_copy(table_in, table, table_sem)
    table_copy.start()
    row_copies = [
        pltpu.make_async_copy(source, rows.at[group], row_sems.at[group])
        for group, source in enumerate(sources)
    ]
    for copy in row_copies:
        copy.start()
    pairs = [(unit_in, unit), (offsets_in, offsets), (weights_in, weights), (atoms_in, atoms)]
    if slot:
        pairs += [(before_in, before), (earlier_in, earlier)]
    side_copies = [
        pltpu.make_async_copy(source, target, side_sems.at[place])
        for place, (source, target) in enumerate(pairs)
    ]
    table_copy.wait()
    count = table[base + COUNT]
    live_points = table[base + POINTS]
    base_atom = table[base + ATOM]
    batch = table[base + BATCH]

    def value_copy(step):
        return pltpu.make_async_copy(
            basis.at[pl.ds(pl.multiple_of(batch * PTS + step * BLOCK, BLOCK), BLOCK), :],
            values_in.at[pl.ds(pl.multiple_of(step * BLOCK, BLOCK), BLOCK), :],
            value_sems.at[step],
        )

    for step in range(STEPS):
        pl.when(step * BLOCK < live_points)(lambda step=step: value_copy(step).start())
    for copy in side_copies:
        copy.start()
    if not slot:
        density[...] = jnp.zeros((2, PTS), jnp.float32)
    for copy in row_copies:
        copy.wait()
    lines = rows.reshape(len(sources) * DEVICES * 8, TILE)

    def unpack(last):
        for first in range(last + 1):
            start = table[base + LINE + pair_start(last) + first]
            words = lines[pl.ds(start, TILE, stride=8), :]
            down = slice(first * TILE, (first + 1) * TILE)
            for matrix in range(2):
                value = words >> 16 if matrix == 0 else (words << 16) >> 16
                value = value.astype(jnp.float32)
                top = value.astype(jnp.bfloat16)
                at = (2 * last + matrix) * TILE
                high_part[down, at : at + TILE] = top
                if first < last:
                    bottom = (value - top.astype(jnp.float32)).astype(jnp.bfloat16)
                    low_part[down, at : at + TILE] = bottom

    for last in range(KT - 2):
        unpack(last)
    for last in range(KT - 2, KT):
        pl.when(count > last)(lambda last=last: unpack(last))
    for copy in side_copies:
        copy.wait()
    if slot:
        which = lax.broadcasted_iota(jnp.int32, (2, PTS), 0)
        for matrix in range(2):
            other = jnp.broadcast_to(earlier[matrix : matrix + 1, :], (2, PTS))
            density[matrix] = jnp.where(which == batch, 0.0, other)

    blocks = (live_points + BLOCK - 1) // BLOCK

    def reduce(step):
        start = pl.multiple_of(step * BLOCK, BLOCK)
        point = start + lax.broadcasted_iota(jnp.int32, (1, BLOCK), 1)
        scale = jnp.where(point < live_points, unit[0:1, 0:1], 0.0)
        at = pl.ds(start, BLOCK)
        for matrix in range(2):
            pieces = [
                jnp.sum(sums_kept[matrix, cut : cut + TILE, :].T, axis=0, keepdims=True)
                for cut in range(0, BLOCK, TILE)
            ]
            line = jnp.concatenate(pieces, axis=1) * scale
            if slot:
                density[matrix, pl.ds(batch, 1), at] = line
            else:
                density[matrix : matrix + 1, at] = line

    def densities(tiles):
        def block(step, carry):
            value_copy(step).wait()
            reduce(jnp.maximum(step - 1, 0))
            start = pl.multiple_of(step * BLOCK, BLOCK)
            columns = []
            for place in range(tiles):
                lane = pl.multiple_of(table[base + place] * TILE, TILE)
                columns.append(values_in[pl.ds(start, BLOCK), pl.ds(lane, TILE)])
            values = jnp.concatenate(columns, axis=1)
            sums = [None, None]
            for last in range(tiles):
                cols = slice(2 * last * TILE, (2 * last + 2) * TILE)
                down = (last + 1) * TILE
                got = jnp.dot(
                    values[:, :down], high_part[:down, cols], preferred_element_type=jnp.float32
                )
                if last:
                    down = last * TILE
                    got = got + jnp.dot(
                        values[:, :down], low_part[:down, cols], preferred_element_type=jnp.float32
                    )
                column = columns[last].astype(jnp.float32)
                for matrix in range(2):
                    part = got[:, matrix * TILE : (matrix + 1) * TILE] * column
                    sums[matrix] = part if last == 0 else sums[matrix] + part
            for matrix in range(2):
                sums_kept[matrix] = sums[matrix]
            return carry

        lax.fori_loop(0, blocks, block, 0)

    for tiles in range(KT - 2, KT + 1):
        pl.when(count == tiles)(lambda tiles=tiles: densities(tiles))
    reduce(jnp.maximum(blocks - 1, 0))

    density_copy = pltpu.make_async_copy(density, density_out, out_sems.at[0])
    density_copy.start()
    mine = pl.ds(batch, 1)
    x = offsets[0, mine, :]
    y = offsets[1, mine, :]
    z = offsets[2, mine, :]
    weight = weights[mine, :]
    near = lax.rem(atoms[mine, :] - base_atom + 2 * ATOMS, ATOMS)
    squared = x * x + y * y + z * z
    shapes = [
        jnp.ones_like(x), x, y, z, x * y, y * z,
        3.0 * z * z - squared, x * z, x * x - y * y,
    ]
    shapes = jnp.concatenate([weight * shape for shape in shapes], axis=0)
    lane = lax.broadcasted_iota(jnp.int32, (9, TILE), 1)
    degree = lax.broadcasted_iota(jnp.int32, (9, TILE), 0)
    lane = lane - degree * SPAN - 4 * batch
    for matrix in range(2):
        terms = density[matrix, mine, :] if slot else density[matrix : matrix + 1, :]
        terms = terms * shapes
        total = jnp.zeros((9, TILE), jnp.float32)
        for atom in range(8):
            picked = jnp.sum(jnp.where(near == atom, terms, 0.0), axis=1, keepdims=True)
            total = total + jnp.where(lane == atom, picked, 0.0)
        line = jnp.sum(total, axis=0, keepdims=True)
        if slot:
            line = line + before[matrix : matrix + 1, :]
            payload[:, matrix : matrix + 1, :] = jnp.broadcast_to(line[None], (DEVICES, 1, TILE))
        else:
            payload[matrix : matrix + 1, :] = line
    payload_copy = pltpu.make_async_copy(payload, payload_out, out_sems.at[1])
    payload_copy.start()
    payload_copy.wait()
    density_copy.wait()


def batch_call(slot, table, rows, carried, unit, offsets, weights, atoms, basis):
    arrays = [table, *rows, *carried, unit, offsets, weights, atoms, basis]
    payload = (DEVICES, 2, TILE) if slot else (2, TILE)
    density = (2, 2, PTS) if slot else (2, PTS)

    def body(*refs):
        batch_body(slot, *refs)

    return pl.pallas_call(
        body,
        in_specs=[pl.BlockSpec(memory_space=pl.ANY) for _ in arrays],
        out_specs=(pl.BlockSpec(memory_space=pl.ANY), pl.BlockSpec(memory_space=pl.ANY)),
        out_shape=(
            jax.ShapeDtypeStruct(density, jnp.float32),
            jax.ShapeDtypeStruct(payload, jnp.float32),
        ),
        scratch_shapes=[
            pltpu.SMEM((2 * ENTRIES,), jnp.int32),
            pltpu.VMEM((KT * TILE, 2 * KT * TILE), jnp.bfloat16),
            pltpu.VMEM(((KT - 1) * TILE, 2 * KT * TILE), jnp.bfloat16),
            pltpu.VMEM((4, DEVICES, 8, TILE), jnp.int32),
            pltpu.VMEM((PTS, KT * TILE), jnp.bfloat16),
            pltpu.VMEM(density, jnp.float32),
            pltpu.VMEM(payload, jnp.float32),
            pltpu.VMEM((8, TILE), jnp.float32),
            pltpu.VMEM((3, 2, PTS), jnp.float32),
            pltpu.VMEM((2, PTS), jnp.float32),
            pltpu.VMEM((2, PTS), jnp.int32),
            pltpu.VMEM((2, TILE), jnp.float32),
            pltpu.VMEM((2, PTS), jnp.float32),
            pltpu.VMEM((2, BLOCK, TILE), jnp.float32),
            pltpu.SemaphoreType.DMA,
            pltpu.SemaphoreType.DMA((4,)),
            pltpu.SemaphoreType.DMA((STEPS,)),
            pltpu.SemaphoreType.DMA((6,)),
            pltpu.SemaphoreType.DMA((2,)),
        ],
        compiler_params=pltpu.CompilerParams(vmem_limit_bytes=60 * 1024 * 1024),
        cost_estimate=pl.CostEstimate(
            flops=26_000_000_000, bytes_accessed=10_000_000, transcendentals=0
        ),
        name=f"batch_density_{slot}",
    )(*arrays)


def moment_body(arrived, out):
    lane = lax.broadcasted_iota(jnp.int32, (8, TILE), 1)
    for matrix in range(2):
        totals = [jnp.zeros((8, TILE), jnp.float32) for _ in range(9)]
        for place in range(16):
            part = arrived[pl.ds(2 * place + matrix, 8, stride=32), :]
            for degree in range(9):
                moved = pltpu.roll(part, (8 * place - SPAN * degree) % TILE, 1)
                if place < 15:
                    mine = (lane >= 8 * place) & (lane < 8 * place + SPAN)
                    totals[degree] = totals[degree] + jnp.where(mine, moved, 0.0)
                else:
                    inside = jnp.where(lane >= 8 * place, moved, 0.0)
                    after = pltpu.roll(jnp.where(lane < SPAN - 8, moved, 0.0), 1, 0)
                    totals[degree] = totals[degree] + inside + after
        for degree in range(9):
            for block in range(8):
                out[degree, matrix : matrix + 1, block * TILE : (block + 1) * TILE] = totals[degree][
                    block : block + 1, :
                ]


def moment_table(arrived):
    return pl.pallas_call(
        moment_body,
        out_shape=jax.ShapeDtypeStruct((9, 2, ATOMS), jnp.float32),
        in_specs=[pl.BlockSpec(memory_space=pltpu.VMEM)],
        out_specs=pl.BlockSpec(memory_space=pltpu.VMEM),
        name="moment_table",
    )(arrived)


def exchange(value):
    return lax.all_to_all(value, ROW_COL, 0, 0, tiled=True)


def local(
    density_first,
    density_second,
    basis,
    tile_list,
    tile_count,
    point_count,
    offsets,
    weights,
    atom_of_point,
):
    rows = spread(tile_list, tile_count, point_count, density_first, density_second)
    rows = exchange(rows.reshape(DEVICES, LINES, TILE)).reshape(DEVICES * LINES, TILE)
    first, rest, unit = windows(rows)
    with jax.named_scope("send_first"):
        first = exchange(first)
    with jax.named_scope("send_rest"):
        rest = exchange(rest)

    table = batch_tables(tile_list, tile_count, point_count)
    flat = basis.reshape(-1, KT * TILE)
    side = (unit, offsets, weights, atom_of_point)
    density_0, payload_0 = batch_call(0, table, (first,), (), *side, flat)
    density, payload = batch_call(
        1, table, (first, rest), (payload_0, density_0), *side, flat
    )
    moments = moment_table(exchange(payload).reshape(DEVICES * 2, TILE)).swapaxes(0, 1)
    return density, moments


def solution(mesh):
    torus = Mesh(mesh.devices.reshape(4, 4, 4, 2), ("row_0", "row_1", "col_0", "col_1"))
    in_specs = (
        P(ROW, COL),
        P(ROW, COL),
        P(ROW_COL, None, None),
        P(ROW_COL, None),
        P(ROW_COL),
        P(ROW_COL),
        P(None, ROW_COL, None),
        P(ROW_COL, None),
        P(ROW_COL, None),
    )
    out_specs = (P(None, ROW_COL, None), P())
    return jax.shard_map(local, mesh=torus, in_specs=in_specs, out_specs=out_specs, check_vma=False)
```

```python
import jax
import jax.numpy as jnp
from jax import lax
from jax.experimental import pallas as pl
from jax.experimental.pallas import tpu as pltpu
from jax.sharding import Mesh
from jax.sharding import PartitionSpec as P

TILE = 128
KT = 7
NT = 96
PTS = 4096
ATOMS = 1024
N_ROW = 16
N_COL = 8
DEVICES = 128
SPAN = 12
ROW = ("row_0", "row_1")
COL = ("col_0", "col_1")
ROW_COL = ("row_0", "row_1", "col_0", "col_1")

SLOTS = 24
LINES = 32
PAIRS = KT * (KT + 1) // 2
WINDOW = 2 * PAIRS
FIRST = 32
REST = WINDOW - FIRST
GROUPS = 4
SLOT_LINES = 24
FRONT = 1152
BACK = 1536
BLOCK = 512
STEPS = PTS // BLOCK
ROUNDER = 12582912.0


def pair_start(last):
    return last * (last + 1) // 2


def spread_body(
    list_in, tiles_in, points_in, first, second, out,
    tiles, lines, tile_list, tile_count, point_count, sems,
):
    my_row = lax.axis_index(ROW)
    my_col = lax.axis_index(COL)
    small = [
        pltpu.make_async_copy(source, target, sems.at[SLOTS + place])
        for place, (source, target) in enumerate(
            ((list_in, tile_list), (tiles_in, tile_count), (points_in, point_count))
        )
    ]
    for copy in small:
        copy.start()
    lead = lax.rem(my_col - my_row + 16, 8)
    base = (my_row - my_col + lead) // 8
    copies = []
    for half in range(2):
        for step in range(6):
            for which, stored in enumerate((first, second)):
                index = which * 12 + half * 6 + step
                column = jnp.clip(2 * step + base - half, 0, 11)
                copy = pltpu.make_async_copy(
                    stored.at[pl.ds(step * TILE, TILE), pl.ds(pl.multiple_of(column * TILE, TILE), TILE)],
                    tiles.at[index],
                    sems.at[index],
                )
                copy.start()
                copies.append((copy, index, half, step))
    largest = jnp.zeros((8, TILE), jnp.float32)
    for copy, index, half, step in copies:
        copy.wait()
        values = tiles[index].astype(jnp.float32)
        column = 2 * step + base - half
        shift = lead - 8 * half
        used = (column >= 0) & (column < 12) & (shift <= 6) & (shift >= -6)
        peak = jnp.max(jnp.abs(values).reshape(16, 8, TILE), axis=0)
        largest = jnp.maximum(largest, jnp.where(used, peak, 0.0))
        if half:
            values = values.T
        lines[pl.ds(index, TILE, stride=SLOTS), :] = values
    for copy in small:
        copy.wait()
    own_start = [least_tile(tile_list, batch) for batch in slot_order(tile_count, point_count)]
    peak = jnp.max(largest)
    line = lax.broadcasted_iota(jnp.int32, (8, TILE), 0)
    extra = jnp.where(
        line == 0,
        own_start[0].astype(jnp.float32),
        jnp.where(line == 1, own_start[1].astype(jnp.float32), peak),
    )

    def pack(dest, carry):
        at = pl.multiple_of(dest * SLOTS, 8)
        low = lines[pl.ds(at, 16), :]
        high = lines[pl.ds(at + 16, 8), :]
        to = pl.multiple_of(dest * LINES, 16)
        out[pl.ds(to, 16), :] = low.astype(jnp.bfloat16)
        out[pl.ds(to + 16, 16), :] = jnp.concatenate([high, extra], axis=0).astype(jnp.bfloat16)
        return carry

    lax.fori_loop(0, DEVICES, pack, 0, unroll=4)


def spread(tile_list, tile_count, point_count, first, second):
    return pl.pallas_call(
        spread_body,
        out_shape=pltpu.VMEM((DEVICES * LINES, TILE), jnp.bfloat16),
        in_specs=[
            pl.BlockSpec(memory_space=pl.ANY),
            pl.BlockSpec(memory_space=pl.ANY),
            pl.BlockSpec(memory_space=pl.ANY),
            pl.BlockSpec(memory_space=pl.ANY),
            pl.BlockSpec(memory_space=pl.ANY),
        ],
        out_specs=pl.BlockSpec(memory_space=pltpu.VMEM),
        scratch_shapes=[
            pltpu.VMEM((SLOTS, TILE, TILE), jnp.bfloat16),
            pltpu.VMEM((DEVICES * SLOTS, TILE), jnp.float32),
            pltpu.SMEM((2, KT), jnp.int32),
            pltpu.SMEM((2,), jnp.int32),
            pltpu.SMEM((2,), jnp.int32),
            pltpu.SemaphoreType.DMA((SLOTS + 3,)),
        ],
        name="spread_rows",
    )(tile_list, tile_count, point_count, first, second)


def window_body(
    arrived, first_out, coded_to, starts_to, unit_to,
    lines, coded, start_lines, starts, out_first, unit_out, sem, out_sems,
):
    def widen(source, top):
        at = pl.multiple_of(source * LINES, 16)
        to = pl.multiple_of(FRONT + source * SLOTS, 8)
        low = arrived[pl.ds(at, 16), :].astype(jnp.float32)
        high = arrived[pl.ds(at + 16, 16), :].astype(jnp.float32)
        lines[pl.ds(to, 16), :] = low
        lines[pl.ds(to + 16, 8), :] = high[0:8]
        extra = high[8:16]
        peak, own = top
        lane = lax.broadcasted_iota(jnp.int32, (8, TILE), 1)
        own = jnp.where(lane == source, extra, own)
        return jnp.maximum(peak, extra), own

    zero = jnp.zeros((8, TILE), jnp.float32)
    tops, own = lax.fori_loop(0, DEVICES, widen, (zero, zero), unroll=4)
    start_lines[...] = own.astype(jnp.int32)
    copy = pltpu.make_async_copy(start_lines, starts, sem)
    copy.start()
    starts_copy = pltpu.make_async_copy(start_lines, starts_to, out_sems.at[2])
    starts_copy.start()
    peak = jnp.broadcast_to(tops[2:3, :], (8, TILE))
    scale = jnp.full((8, TILE), 2.0**21, jnp.float32)
    unit = jnp.full((8, TILE), 2.0**-21, jnp.float32)
    for step in range(1, 64):
        small = peak < 2.0 ** (-7 - step)
        scale = jnp.where(small, 2.0 ** (21 + step), scale)
        unit = jnp.where(small, 2.0 ** (-21 - step), unit)
    unit_out[...] = unit
    unit_copy = pltpu.make_async_copy(unit_out, unit_to, out_sems.at[0])
    unit_copy.start()

    order = lax.broadcasted_iota(jnp.int32, (8, TILE), 0)

    def line_of(row, col, which, half, step):
        return FRONT + (row * N_COL + col) * SLOTS + which * 12 + half * 6 + step

    def eight(start):
        return lines[pl.ds(start, 8, stride=(N_COL + 1) * SLOTS), :]

    for apart in range(KT):
        for group in range(NT // 8):
            words = []
            for which in range(2):
                odd = group % 2
                step = group // 2
                if odd or apart == 0:
                    total = eight(line_of(8 * odd - apart, 0, which, 0, step))
                else:
                    total = eight(line_of(-apart, 0, which, 0, step))
                    if step > 0:
                        before = eight(line_of(16 - apart, 0, which, 0, step - 1))
                        total = jnp.where(order < apart, before, total)
                if apart > 0:
                    after = eight(line_of(8 * odd, -apart, which, 1, step))
                    wrapped = eight(line_of(8 * odd, 8 - apart, which, 1, step))
                    total = total + jnp.where(order < apart, wrapped, after)
                total = total * scale
                words.append(((total + ROUNDER) - ROUNDER).astype(jnp.int32))
            word = (words[0] << 16) | (words[1] & 0xFFFF)
            coded[pl.ds(group * 64 + apart, 8, stride=8), :] = word

    coded_copy = pltpu.make_async_copy(coded, coded_to, out_sems.at[1])
    coded_copy.start()
    copy.wait()
    copies = fill_windows(starts, coded, out_first, first_out, 0, FIRST, out_sems)
    for copy in [unit_copy, starts_copy, coded_copy, *copies]:
        copy.wait()


def fill_windows(starts, coded, filled, out, begin, end, sems):
    def fill(dest, carry):
        for slot in range(2):
            start = starts[slot, dest]
            for last in range(KT):
                low = slot * PAIRS + pair_start(last)
                high = low + last + 1
                top = max(low, begin)
                bottom = min(high, end)
                if top < bottom:
                    words = coded[pl.ds(pl.multiple_of((start + last) * 8, 8), 8), :]
                    filled[dest, top - begin : bottom - begin, :] = words[top - low : bottom - low]
        return carry

    copies = []
    group = DEVICES // GROUPS
    for part in range(GROUPS):
        lax.fori_loop(part * group, (part + 1) * group, fill, 0, unroll=2)
        span = pl.ds(part * group, group)
        copy = pltpu.make_async_copy(filled.at[span], out.at[span], sems.at[3 + part])
        copy.start()
        copies.append(copy)
    return copies


def windows(arrived):
    return pl.pallas_call(
        window_body,
        out_shape=(
            pltpu.HBM((DEVICES, FIRST, TILE), jnp.int32),
            pltpu.HBM((NT * 8, TILE), jnp.int32),
            pltpu.HBM((8, TILE), jnp.int32),
            pltpu.HBM((8, TILE), jnp.float32),
        ),
        in_specs=[pl.BlockSpec(memory_space=pltpu.VMEM)],
        out_specs=tuple(pl.BlockSpec(memory_space=pl.ANY) for _ in range(4)),
        scratch_shapes=[
            pltpu.VMEM((FRONT + DEVICES * SLOTS + BACK, TILE), jnp.float32),
            pltpu.VMEM((NT * 8, TILE), jnp.int32),
            pltpu.VMEM((8, TILE), jnp.int32),
            pltpu.SMEM((8, TILE), jnp.int32),
            pltpu.VMEM((DEVICES, FIRST, TILE), jnp.int32),
            pltpu.VMEM((8, TILE), jnp.float32),
            pltpu.SemaphoreType.DMA,
            pltpu.SemaphoreType.DMA((3 + GROUPS,)),
        ],
        compiler_params=pltpu.CompilerParams(vmem_limit_bytes=24 * 1024 * 1024),
        name="pick_windows",
    )(arrived)


def rest_body(starts, coded, out, filled, sems):
    for copy in fill_windows(starts, coded, filled, out, FIRST, WINDOW, sems):
        copy.wait()


def rest_windows(starts, coded):
    return pl.pallas_call(
        rest_body,
        out_shape=jax.ShapeDtypeStruct((DEVICES, REST, TILE), jnp.int32),
        in_specs=[
            pl.BlockSpec(memory_space=pltpu.SMEM),
            pl.BlockSpec(memory_space=pltpu.VMEM),
        ],
        out_specs=pl.BlockSpec(memory_space=pl.ANY),
        scratch_shapes=[
            pltpu.VMEM((DEVICES, REST, TILE), jnp.int32),
            pltpu.SemaphoreType.DMA((3 + GROUPS,)),
        ],
        name="pick_rest",
    )(starts, coded)


def slot_order(tile_count, point_count):
    work = []
    for batch in range(2):
        count = tile_count[batch]
        passes = jnp.where(count >= KT, 28, jnp.where(count == KT - 1, 21, 15))
        work.append(passes * point_count[batch])
    swap = (work[1] > work[0]).astype(jnp.int32)
    return swap, 1 - swap


def least_tile(tile_list, batch):
    least = tile_list[batch, 0]
    for place in range(1, KT):
        least = jnp.minimum(least, tile_list[batch, place])
    return least


COUNT = 7
POINTS = 8
ATOM = 9
BATCH = 10
LINE = 11
ENTRIES = 40


def table_body(tile_list, tile_count, point_count, table, column_of, order_of):
    device = lax.axis_index(ROW) * N_COL + lax.axis_index(COL)
    for slot, batch in enumerate(slot_order(tile_count, point_count)):
        base = slot * ENTRIES
        start = least_tile(tile_list, batch)
        count = jnp.minimum(tile_count[batch], KT)
        for place in range(KT):
            column_of[tile_list[batch, place] - start] = place
        live_end = 0
        dead_end = count
        for rank in range(KT):
            place = column_of[rank]
            live = (place < count).astype(jnp.int32)
            to = jnp.where(live == 1, live_end, dead_end)
            table[base + to] = place
            order_of[to] = rank
            live_end = live_end + live
            dead_end = dead_end + 1 - live
        table[base + COUNT] = count
        table[base + POINTS] = point_count[batch]
        table[base + ATOM] = lax.rem((2 * device + batch) * 4, ATOMS)
        table[base + BATCH] = batch
        for last in range(KT):
            high = order_of[last]
            for first in range(last + 1):
                low = order_of[first]
                line = slot * (PAIRS - SLOT_LINES) + high * (high + 1) // 2 + high - low
                line = jnp.where(last < count, line, SLOT_LINES)
                table[base + LINE + pair_start(last) + first] = (line // 8) * (DEVICES * 8) + line % 8


def batch_tables(tile_list, tile_count, point_count):
    return pl.pallas_call(
        table_body,
        out_shape=jax.ShapeDtypeStruct((2 * ENTRIES,), jnp.int32),
        in_specs=[pl.BlockSpec(memory_space=pltpu.SMEM) for _ in range(3)],
        out_specs=pl.BlockSpec(memory_space=pltpu.SMEM),
        scratch_shapes=[pltpu.SMEM((8,), jnp.int32), pltpu.SMEM((8,), jnp.int32)],
        name="batch_tables",
    )(tile_list, tile_count, point_count)


def batch_body(slot, *refs):
    table_in, first_rows = refs[:2]
    refs = refs[2:]
    if slot:
        rest_rows, before_in, earlier_in = refs[:3]
        refs = refs[3:]
        sources = [first_rows.at[:, pl.ds(FIRST - 8, 8), :]]
        sources += [rest_rows.at[:, pl.ds(8 * group, 8), :] for group in range(REST // 8)]
    else:
        sources = [first_rows.at[:, pl.ds(8 * group, 8), :] for group in range(FIRST // 8)]
    unit_in, offsets_in, weights_in, atoms_in, basis, density_out, payload_out = refs[:7]
    (
        table, parts, rows, values_in, density, payload,
        unit, offsets, weights, atoms, before, earlier, sums_kept,
        table_sem, row_sems, value_sems, side_sems, out_sems,
    ) = refs[7:]
    base = slot * ENTRIES
    if slot:
        payload = payload_out

    table_copy = pltpu.make_async_copy(table_in, table, table_sem)
    table_copy.start()
    row_copies = [
        pltpu.make_async_copy(source, rows.at[group], row_sems.at[group])
        for group, source in enumerate(sources)
    ]
    for copy in row_copies:
        copy.start()
    pairs = [(unit_in, unit), (offsets_in, offsets), (weights_in, weights), (atoms_in, atoms)]
    if slot:
        pairs += [(before_in, before), (earlier_in, earlier)]
    side_copies = [
        pltpu.make_async_copy(source, target, side_sems.at[place])
        for place, (source, target) in enumerate(pairs)
    ]
    table_copy.wait()
    count = table[base + COUNT]
    live_points = table[base + POINTS]
    base_atom = table[base + ATOM]
    batch = table[base + BATCH]

    def value_copy(step):
        return pltpu.make_async_copy(
            basis.at[pl.ds(pl.multiple_of(batch * PTS + step * BLOCK, BLOCK), BLOCK), :],
            values_in.at[pl.ds(pl.multiple_of(step * BLOCK, BLOCK), BLOCK), :],
            value_sems.at[step],
        )

    for step in range(STEPS):
        pl.when(step * BLOCK < live_points)(lambda step=step: value_copy(step).start())
    for copy in side_copies:
        copy.start()
    if not slot:
        density[...] = jnp.zeros((2, PTS), jnp.float32)
    for copy in row_copies:
        copy.wait()
    lines = rows.reshape(len(sources) * DEVICES * 8, TILE)

    def unpack(last):
        for first in range(last + 1):
            start = table[base + LINE + pair_start(last) + first]
            words = lines[pl.ds(start, TILE, stride=8), :]
            down = slice(first * TILE, (first + 1) * TILE)
            for matrix in range(2):
                value = words >> 16 if matrix == 0 else (words << 16) >> 16
                value = value.astype(jnp.float32)
                top = value.astype(jnp.bfloat16)
                at = (2 * last + matrix) * TILE
                parts[down, at : at + TILE] = top
                if first < last:
                    bottom = (value - top.astype(jnp.float32)).astype(jnp.bfloat16)
                    parts[(last + 1 + first) * TILE : (last + 2 + first) * TILE, at : at + TILE] = bottom

    for last in range(KT - 2):
        unpack(last)
    for last in range(KT - 2, KT):
        pl.when(count > last)(lambda last=last: unpack(last))
    for copy in side_copies:
        copy.wait()
    if slot:
        which = lax.broadcasted_iota(jnp.int32, (2, PTS), 0)
        for matrix in range(2):
            other = jnp.broadcast_to(earlier[matrix : matrix + 1, :], (2, PTS))
            density[matrix] = jnp.where(which == batch, 0.0, other)

    blocks = (live_points + BLOCK - 1) // BLOCK

    def reduce(step):
        start = pl.multiple_of(step * BLOCK, BLOCK)
        point = start + lax.broadcasted_iota(jnp.int32, (1, BLOCK), 1)
        scale = jnp.where(point < live_points, unit[0:1, 0:1], 0.0)
        at = pl.ds(start, BLOCK)
        for matrix in range(2):
            pieces = [
                jnp.sum(sums_kept[matrix, cut : cut + TILE, :].T, axis=0, keepdims=True)
                for cut in range(0, BLOCK, TILE)
            ]
            line = jnp.concatenate(pieces, axis=1) * scale
            if slot:
                density[matrix, pl.ds(batch, 1), at] = line
            else:
                density[matrix : matrix + 1, at] = line

    def densities(tiles):
        def block(step, carry):
            value_copy(step).wait()
            reduce(jnp.maximum(step - 1, 0))
            start = pl.multiple_of(step * BLOCK, BLOCK)
            columns = []
            for place in range(tiles):
                lane = pl.multiple_of(table[base + place] * TILE, TILE)
                columns.append(values_in[pl.ds(start, BLOCK), pl.ds(lane, TILE)])
            values = jnp.concatenate(columns, axis=1)
            sums = [None, None]
            for last in range(tiles):
                cols = slice(2 * last * TILE, (2 * last + 2) * TILE)
                down = (last + 1) * TILE
                both = jnp.concatenate(columns[: last + 1] + columns[:last], axis=1)
                got = jnp.dot(
                    both, parts[: (2 * last + 1) * TILE, cols], preferred_element_type=jnp.float32
                )
                column = columns[last].astype(jnp.float32)
                for matrix in range(2):
                    part = got[:, matrix * TILE : (matrix + 1) * TILE] * column
                    sums[matrix] = part if last == 0 else sums[matrix] + part
            for matrix in range(2):
                sums_kept[matrix] = sums[matrix]
            return carry

        lax.fori_loop(0, blocks, block, 0)

    for tiles in range(KT - 2, KT + 1):
        pl.when(count == tiles)(lambda tiles=tiles: densities(tiles))
    reduce(jnp.maximum(blocks - 1, 0))

    density_copy = pltpu.make_async_copy(density, density_out, out_sems.at[0])
    density_copy.start()
    mine = pl.ds(batch, 1)
    x = offsets[0, mine, :]
    y = offsets[1, mine, :]
    z = offsets[2, mine, :]
    weight = weights[mine, :]
    near = lax.rem(atoms[mine, :] - base_atom + 2 * ATOMS, ATOMS)
    squared = x * x + y * y + z * z
    shapes = [
        jnp.ones_like(x), x, y, z, x * y, y * z,
        3.0 * z * z - squared, x * z, x * x - y * y,
    ]
    shapes = jnp.concatenate([weight * shape for shape in shapes], axis=0)
    lane = lax.broadcasted_iota(jnp.int32, (9, TILE), 1)
    degree = lax.broadcasted_iota(jnp.int32, (9, TILE), 0)
    lane = lane - degree * SPAN - 4 * batch
    for matrix in range(2):
        terms = density[matrix, mine, :] if slot else density[matrix : matrix + 1, :]
        terms = terms * shapes
        total = jnp.zeros((9, TILE), jnp.float32)
        for atom in range(8):
            picked = jnp.sum(jnp.where(near == atom, terms, 0.0), axis=1, keepdims=True)
            total = total + jnp.where(lane == atom, picked, 0.0)
        line = jnp.sum(total, axis=0, keepdims=True)
        if slot:
            line = line + before[matrix : matrix + 1, :]
            payload[:, matrix : matrix + 1, :] = jnp.broadcast_to(line[None], (DEVICES, 1, TILE))
        else:
            payload[matrix : matrix + 1, :] = line
    if not slot:
        payload_copy = pltpu.make_async_copy(payload, payload_out, out_sems.at[1])
        payload_copy.start()
        payload_copy.wait()
    density_copy.wait()


def batch_call(slot, table, rows, carried, unit, offsets, weights, atoms, basis):
    arrays = [table, *rows, *carried, unit, offsets, weights, atoms, basis]
    payload = (DEVICES, 2, TILE) if slot else (2, TILE)
    density = (2, 2, PTS) if slot else (2, PTS)

    def body(*refs):
        batch_body(slot, *refs)

    return pl.pallas_call(
        body,
        in_specs=[pl.BlockSpec(memory_space=pl.ANY) for _ in arrays],
        out_specs=(
            pl.BlockSpec(memory_space=pl.ANY),
            pl.BlockSpec(memory_space=pltpu.VMEM if slot else pl.ANY),
        ),
        out_shape=(
            jax.ShapeDtypeStruct(density, jnp.float32),
            pltpu.VMEM(payload, jnp.float32) if slot else jax.ShapeDtypeStruct(payload, jnp.float32),
        ),
        scratch_shapes=[
            pltpu.SMEM((2 * ENTRIES,), jnp.int32),
            pltpu.VMEM(((2 * KT - 1) * TILE, 2 * KT * TILE), jnp.bfloat16),
            pltpu.VMEM((4, DEVICES, 8, TILE), jnp.int32),
            pltpu.VMEM((PTS, KT * TILE), jnp.bfloat16),
            pltpu.VMEM(density, jnp.float32),
            pltpu.VMEM((8, TILE) if slot else payload, jnp.float32),
            pltpu.VMEM((8, TILE), jnp.float32),
            pltpu.VMEM((3, 2, PTS), jnp.float32),
            pltpu.VMEM((2, PTS), jnp.float32),
            pltpu.VMEM((2, PTS), jnp.int32),
            pltpu.VMEM((2, TILE), jnp.float32),
            pltpu.VMEM((2, PTS), jnp.float32),
            pltpu.VMEM((2, BLOCK, TILE), jnp.float32),
            pltpu.SemaphoreType.DMA,
            pltpu.SemaphoreType.DMA((4,)),
            pltpu.SemaphoreType.DMA((STEPS,)),
            pltpu.SemaphoreType.DMA((6,)),
            pltpu.SemaphoreType.DMA((2,)),
        ],
        compiler_params=pltpu.CompilerParams(vmem_limit_bytes=60 * 1024 * 1024),
        cost_estimate=pl.CostEstimate(
            flops=26_000_000_000, bytes_accessed=10_000_000, transcendentals=0
        ),
        name=f"batch_density_{slot}",
    )(*arrays)


def moment_body(arrived, out):
    lane = lax.broadcasted_iota(jnp.int32, (8, TILE), 1)
    for matrix in range(2):
        totals = [jnp.zeros((8, TILE), jnp.float32) for _ in range(9)]
        for place in range(16):
            part = arrived[pl.ds(2 * place + matrix, 8, stride=32), :]
            for degree in range(9):
                moved = pltpu.roll(part, (8 * place - SPAN * degree) % TILE, 1)
                if place < 15:
                    mine = (lane >= 8 * place) & (lane < 8 * place + SPAN)
                    totals[degree] = totals[degree] + jnp.where(mine, moved, 0.0)
                else:
                    inside = jnp.where(lane >= 8 * place, moved, 0.0)
                    after = pltpu.roll(jnp.where(lane < SPAN - 8, moved, 0.0), 1, 0)
                    totals[degree] = totals[degree] + inside + after
        for degree in range(9):
            for block in range(8):
                out[degree, matrix : matrix + 1, block * TILE : (block + 1) * TILE] = totals[degree][
                    block : block + 1, :
                ]


def moment_table(arrived):
    return pl.pallas_call(
        moment_body,
        out_shape=jax.ShapeDtypeStruct((9, 2, ATOMS), jnp.float32),
        in_specs=[pl.BlockSpec(memory_space=pltpu.VMEM)],
        out_specs=pl.BlockSpec(memory_space=pltpu.VMEM),
        compiler_params=pltpu.CompilerParams(vmem_limit_bytes=8 * 1024 * 1024),
        name="moment_table",
    )(arrived)


def exchange(value):
    return lax.all_to_all(value, ROW_COL, 0, 0, tiled=True)


def local(
    density_first,
    density_second,
    basis,
    tile_list,
    tile_count,
    point_count,
    offsets,
    weights,
    atom_of_point,
):
    rows = spread(tile_list, tile_count, point_count, density_first, density_second)
    rows = exchange(rows.reshape(DEVICES, LINES, TILE)).reshape(DEVICES * LINES, TILE)
    first, coded, starts, unit = windows(rows)
    first = exchange(first)
    rest = exchange(rest_windows(starts, coded))

    table = batch_tables(tile_list, tile_count, point_count)
    flat = basis.reshape(-1, KT * TILE)
    side = (unit, offsets, weights, atom_of_point)
    density_0, payload_0 = batch_call(0, table, (first,), (), *side, flat)
    density, payload = batch_call(
        1, table, (first, rest), (payload_0, density_0), *side, flat
    )
    moments = moment_table(exchange(payload).reshape(DEVICES * 2, TILE)).swapaxes(0, 1)
    return density, moments


def solution(mesh):
    torus = Mesh(mesh.devices.reshape(4, 4, 4, 2), ("row_0", "row_1", "col_0", "col_1"))
    in_specs = (
        P(ROW, COL),
        P(ROW, COL),
        P(ROW_COL, None, None),
        P(ROW_COL, None),
        P(ROW_COL),
        P(ROW_COL),
        P(None, ROW_COL, None),
        P(ROW_COL, None),
        P(ROW_COL, None),
    )
    out_specs = (P(None, ROW_COL, None), P())
    return jax.shard_map(local, mesh=torus, in_specs=in_specs, out_specs=out_specs, check_vma=False)
```

```python
import jax
import jax.numpy as jnp
from jax import lax
from jax.experimental import pallas as pl
from jax.experimental.pallas import tpu as pltpu
from jax.sharding import Mesh
from jax.sharding import PartitionSpec as P

TILE = 128
KT = 7
NT = 96
PTS = 4096
ATOMS = 1024
N_ROW = 16
N_COL = 8
DEVICES = 128
SPAN = 12
ROW = ("row_0", "row_1")
COL = ("col_0", "col_1")
ROW_COL = ("row_0", "row_1", "col_0", "col_1")

SLOTS = 24
LINES = 32
PAIRS = KT * (KT + 1) // 2
WINDOW = 2 * PAIRS
GROUPS = 4
FRONT = 1152
BACK = 1536
BLOCK = 512
STEPS = PTS // BLOCK
ROUNDER = 12582912.0


def pair_start(last):
    return last * (last + 1) // 2


def spread_body(
    list_in, tiles_in, points_in, first, second, out,
    tiles, lines, tile_list, tile_count, point_count, sems,
):
    my_row = lax.axis_index(ROW)
    my_col = lax.axis_index(COL)
    small = [
        pltpu.make_async_copy(source, target, sems.at[SLOTS + place])
        for place, (source, target) in enumerate(
            ((list_in, tile_list), (tiles_in, tile_count), (points_in, point_count))
        )
    ]
    for copy in small:
        copy.start()
    lead = lax.rem(my_col - my_row + 16, 8)
    base = (my_row - my_col + lead) // 8
    copies = []
    for half in range(2):
        for step in range(6):
            for which, stored in enumerate((first, second)):
                index = which * 12 + half * 6 + step
                column = jnp.clip(2 * step + base - half, 0, 11)
                copy = pltpu.make_async_copy(
                    stored.at[pl.ds(step * TILE, TILE), pl.ds(pl.multiple_of(column * TILE, TILE), TILE)],
                    tiles.at[index],
                    sems.at[index],
                )
                copy.start()
                copies.append((copy, index, half, step))
    largest = jnp.zeros((8, TILE), jnp.float32)
    for copy, index, half, step in copies:
        copy.wait()
        values = tiles[index].astype(jnp.float32)
        column = 2 * step + base - half
        shift = lead - 8 * half
        used = (column >= 0) & (column < 12) & (shift <= 6) & (shift >= -6)
        peak = jnp.max(jnp.abs(values).reshape(16, 8, TILE), axis=0)
        largest = jnp.maximum(largest, jnp.where(used, peak, 0.0))
        if half:
            values = values.T
        lines[pl.ds(index, TILE, stride=SLOTS), :] = values
    for copy in small:
        copy.wait()
    own_start = [least_tile(tile_list, batch) for batch in slot_order(tile_count, point_count)]
    peak = jnp.max(largest)
    line = lax.broadcasted_iota(jnp.int32, (8, TILE), 0)
    extra = jnp.where(
        line == 0,
        own_start[0].astype(jnp.float32),
        jnp.where(line == 1, own_start[1].astype(jnp.float32), peak),
    )

    def pack(dest, carry):
        at = pl.multiple_of(dest * SLOTS, 8)
        low = lines[pl.ds(at, 16), :]
        high = lines[pl.ds(at + 16, 8), :]
        to = pl.multiple_of(dest * LINES, 16)
        out[pl.ds(to, 16), :] = low.astype(jnp.bfloat16)
        out[pl.ds(to + 16, 16), :] = jnp.concatenate([high, extra], axis=0).astype(jnp.bfloat16)
        return carry

    lax.fori_loop(0, DEVICES, pack, 0, unroll=4)


def spread(tile_list, tile_count, point_count, first, second):
    return pl.pallas_call(
        spread_body,
        out_shape=pltpu.VMEM((DEVICES * LINES, TILE), jnp.bfloat16),
        in_specs=[
            pl.BlockSpec(memory_space=pl.ANY),
            pl.BlockSpec(memory_space=pl.ANY),
            pl.BlockSpec(memory_space=pl.ANY),
            pl.BlockSpec(memory_space=pl.ANY),
            pl.BlockSpec(memory_space=pl.ANY),
        ],
        out_specs=pl.BlockSpec(memory_space=pltpu.VMEM),
        scratch_shapes=[
            pltpu.VMEM((SLOTS, TILE, TILE), jnp.bfloat16),
            pltpu.VMEM((DEVICES * SLOTS, TILE), jnp.float32),
            pltpu.SMEM((2, KT), jnp.int32),
            pltpu.SMEM((2,), jnp.int32),
            pltpu.SMEM((2,), jnp.int32),
            pltpu.SemaphoreType.DMA((SLOTS + 3,)),
        ],
        name="spread_rows",
    )(tile_list, tile_count, point_count, first, second)


def window_body(
    arrived, first_out, coded_to, starts_to, unit_to,
    lines, coded, start_lines, starts, out_first, unit_out, sem, out_sems,
):
    def widen(source, top):
        at = pl.multiple_of(source * LINES, 16)
        to = pl.multiple_of(FRONT + source * SLOTS, 8)
        low = arrived[pl.ds(at, 16), :].astype(jnp.float32)
        high = arrived[pl.ds(at + 16, 16), :].astype(jnp.float32)
        lines[pl.ds(to, 16), :] = low
        lines[pl.ds(to + 16, 8), :] = high[0:8]
        extra = high[8:16]
        peak, own = top
        lane = lax.broadcasted_iota(jnp.int32, (8, TILE), 1)
        own = jnp.where(lane == source, extra, own)
        return jnp.maximum(peak, extra), own

    zero = jnp.zeros((8, TILE), jnp.float32)
    tops, own = lax.fori_loop(0, DEVICES, widen, (zero, zero), unroll=4)
    start_lines[...] = own.astype(jnp.int32)
    copy = pltpu.make_async_copy(start_lines, starts, sem)
    copy.start()
    starts_copy = pltpu.make_async_copy(start_lines, starts_to, out_sems.at[2])
    starts_copy.start()
    peak = jnp.broadcast_to(tops[2:3, :], (8, TILE))
    scale = jnp.full((8, TILE), 2.0**21, jnp.float32)
    unit = jnp.full((8, TILE), 2.0**-21, jnp.float32)
    for step in range(1, 64):
        small = peak < 2.0 ** (-7 - step)
        scale = jnp.where(small, 2.0 ** (21 + step), scale)
        unit = jnp.where(small, 2.0 ** (-21 - step), unit)
    unit_out[...] = unit
    unit_copy = pltpu.make_async_copy(unit_out, unit_to, out_sems.at[0])
    unit_copy.start()

    order = lax.broadcasted_iota(jnp.int32, (8, TILE), 0)

    def line_of(row, col, which, half, step):
        return FRONT + (row * N_COL + col) * SLOTS + which * 12 + half * 6 + step

    def eight(start):
        return lines[pl.ds(start, 8, stride=(N_COL + 1) * SLOTS), :]

    for apart in range(KT):
        for group in range(NT // 8):
            words = []
            for which in range(2):
                odd = group % 2
                step = group // 2
                if odd or apart == 0:
                    total = eight(line_of(8 * odd - apart, 0, which, 0, step))
                else:
                    total = eight(line_of(-apart, 0, which, 0, step))
                    if step > 0:
                        before = eight(line_of(16 - apart, 0, which, 0, step - 1))
                        total = jnp.where(order < apart, before, total)
                if apart > 0:
                    after = eight(line_of(8 * odd, -apart, which, 1, step))
                    wrapped = eight(line_of(8 * odd, 8 - apart, which, 1, step))
                    total = total + jnp.where(order < apart, wrapped, after)
                total = total * scale
                words.append(((total + ROUNDER) - ROUNDER).astype(jnp.int32))
            word = (words[0] << 16) | (words[1] & 0xFFFF)
            coded[pl.ds(group * 64 + apart, 8, stride=8), :] = word

    coded_copy = pltpu.make_async_copy(coded, coded_to, out_sems.at[1])
    coded_copy.start()
    copy.wait()
    copies = fill_windows(0, starts, coded, out_first, first_out, out_sems)
    for copy in [unit_copy, starts_copy, coded_copy, *copies]:
        copy.wait()


def fill_windows(slot, starts, coded, filled, out, sems):
    def fill(pair, carry):
        for half in range(2):
            start = starts[slot, 2 * pair + half]
            for last in range(KT):
                words = coded[pl.ds(pl.multiple_of((start + last) * 8, 8), 8), :]
                low = half * PAIRS + pair_start(last)
                filled[pair, low : low + last + 1, :] = words[: last + 1]
        return carry

    copies = []
    group = DEVICES // 2 // GROUPS
    for part in range(GROUPS):
        lax.fori_loop(part * group, (part + 1) * group, fill, 0, unroll=2)
        span = pl.ds(part * group, group)
        copy = pltpu.make_async_copy(filled.at[span], out.at[span], sems.at[3 + part])
        copy.start()
        copies.append(copy)
    return copies


def windows(arrived):
    return pl.pallas_call(
        window_body,
        out_shape=(
            pltpu.HBM((DEVICES // 2, WINDOW, TILE), jnp.int32),
            pltpu.HBM((NT * 8, TILE), jnp.int32),
            pltpu.HBM((8, TILE), jnp.int32),
            pltpu.HBM((8, TILE), jnp.float32),
        ),
        in_specs=[pl.BlockSpec(memory_space=pltpu.VMEM)],
        out_specs=tuple(pl.BlockSpec(memory_space=pl.ANY) for _ in range(4)),
        scratch_shapes=[
            pltpu.VMEM((FRONT + DEVICES * SLOTS + BACK, TILE), jnp.float32),
            pltpu.VMEM((NT * 8, TILE), jnp.int32),
            pltpu.VMEM((8, TILE), jnp.int32),
            pltpu.SMEM((8, TILE), jnp.int32),
            pltpu.VMEM((DEVICES // 2, WINDOW, TILE), jnp.int32),
            pltpu.VMEM((8, TILE), jnp.float32),
            pltpu.SemaphoreType.DMA,
            pltpu.SemaphoreType.DMA((3 + GROUPS,)),
        ],
        compiler_params=pltpu.CompilerParams(vmem_limit_bytes=24 * 1024 * 1024),
        name="pick_windows",
    )(arrived)


def rest_body(starts, coded, out, filled, sems):
    for copy in fill_windows(1, starts, coded, filled, out, sems):
        copy.wait()


def rest_windows(starts, coded):
    return pl.pallas_call(
        rest_body,
        out_shape=jax.ShapeDtypeStruct((DEVICES // 2, WINDOW, TILE), jnp.int32),
        in_specs=[
            pl.BlockSpec(memory_space=pltpu.SMEM),
            pl.BlockSpec(memory_space=pltpu.VMEM),
        ],
        out_specs=pl.BlockSpec(memory_space=pl.ANY),
        scratch_shapes=[
            pltpu.VMEM((DEVICES // 2, WINDOW, TILE), jnp.int32),
            pltpu.SemaphoreType.DMA((3 + GROUPS,)),
        ],
        name="pick_rest",
    )(starts, coded)


def slot_order(tile_count, point_count):
    work = []
    for batch in range(2):
        count = tile_count[batch]
        passes = jnp.where(count >= KT, 28, jnp.where(count == KT - 1, 21, 15))
        work.append(passes * point_count[batch])
    swap = (work[1] > work[0]).astype(jnp.int32)
    return swap, 1 - swap


def least_tile(tile_list, batch):
    least = tile_list[batch, 0]
    for place in range(1, KT):
        least = jnp.minimum(least, tile_list[batch, place])
    return least


COUNT = 7
POINTS = 8
ATOM = 9
BATCH = 10
LINE = 11
ENTRIES = 40


def table_body(tile_list, tile_count, point_count, table, column_of, order_of):
    device = lax.axis_index(ROW) * N_COL + lax.axis_index(COL)
    for slot, batch in enumerate(slot_order(tile_count, point_count)):
        base = slot * ENTRIES
        start = least_tile(tile_list, batch)
        count = jnp.minimum(tile_count[batch], KT)
        for place in range(KT):
            column_of[tile_list[batch, place] - start] = place
        live_end = 0
        dead_end = count
        for rank in range(KT):
            place = column_of[rank]
            live = (place < count).astype(jnp.int32)
            to = jnp.where(live == 1, live_end, dead_end)
            table[base + to] = place
            order_of[to] = rank
            live_end = live_end + live
            dead_end = dead_end + 1 - live
        table[base + COUNT] = count
        table[base + POINTS] = point_count[batch]
        table[base + ATOM] = lax.rem((2 * device + batch) * 4, ATOMS)
        table[base + BATCH] = batch
        for last in range(KT):
            high = order_of[last]
            for first in range(last + 1):
                low = order_of[first]
                line = high * (high + 1) // 2 + high - low
                table[base + LINE + pair_start(last) + first] = jnp.where(last < count, line, 0)


def batch_tables(tile_list, tile_count, point_count):
    return pl.pallas_call(
        table_body,
        out_shape=jax.ShapeDtypeStruct((2 * ENTRIES,), jnp.int32),
        in_specs=[pl.BlockSpec(memory_space=pltpu.SMEM) for _ in range(3)],
        out_specs=pl.BlockSpec(memory_space=pltpu.SMEM),
        scratch_shapes=[pltpu.SMEM((8,), jnp.int32), pltpu.SMEM((8,), jnp.int32)],
        name="batch_tables",
    )(tile_list, tile_count, point_count)


def batch_body(slot, *refs):
    table, rows = refs[:2]
    refs = refs[2:]
    if slot:
        before, earlier = refs[:2]
        refs = refs[2:]
    unit, offsets, weights, atoms, basis, density_out, payload = refs[:7]
    parts, values_in, density, sums_kept = refs[7:11]
    value_sems, out_sems = refs[11:13]
    base = slot * ENTRIES
    if slot:
        rows_here, row_sems = refs[13:]
        row_copies = []
        for group in range(4):
            span = pl.ds(group * (DEVICES * PAIRS // 4), DEVICES * PAIRS // 4)
            row_copies.append(
                pltpu.make_async_copy(rows.at[span], rows_here.at[span], row_sems.at[group])
            )
        for copy in row_copies:
            copy.start()
        rows = rows_here
    count = table[base + COUNT]
    live_points = table[base + POINTS]
    base_atom = table[base + ATOM]
    batch = table[base + BATCH]

    def value_copy(step):
        return pltpu.make_async_copy(
            basis.at[pl.ds(pl.multiple_of(batch * PTS + step * BLOCK, BLOCK), BLOCK), :],
            values_in.at[pl.ds(pl.multiple_of(step * BLOCK, BLOCK), BLOCK), :],
            value_sems.at[step],
        )

    for step in range(STEPS):
        pl.when(step * BLOCK < live_points)(lambda step=step: value_copy(step).start())
    if slot:
        for copy in row_copies:
            copy.wait()
    else:
        density[...] = jnp.zeros((2, PTS), jnp.float32)

    def unpack(last):
        for first in range(last + 1):
            start = table[base + LINE + pair_start(last) + first]
            words = rows[pl.ds(start, TILE, stride=PAIRS), :]
            down = slice(first * TILE, (first + 1) * TILE)
            for matrix in range(2):
                value = words >> 16 if matrix == 0 else (words << 16) >> 16
                value = value.astype(jnp.float32)
                top = value.astype(jnp.bfloat16)
                at = (2 * last + matrix) * TILE
                parts[down, at : at + TILE] = top
                if first < last:
                    bottom = (value - top.astype(jnp.float32)).astype(jnp.bfloat16)
                    parts[(last + 1 + first) * TILE : (last + 2 + first) * TILE, at : at + TILE] = bottom

    for last in range(KT - 2):
        unpack(last)
    for last in range(KT - 2, KT):
        pl.when(count > last)(lambda last=last: unpack(last))
    if slot:
        which = lax.broadcasted_iota(jnp.int32, (2, PTS), 0)
        for matrix in range(2):
            other = jnp.broadcast_to(earlier[matrix : matrix + 1, :], (2, PTS))
            density[matrix] = jnp.where(which == batch, 0.0, other)

    blocks = (live_points + BLOCK - 1) // BLOCK

    def reduce(step):
        start = pl.multiple_of(step * BLOCK, BLOCK)
        point = start + lax.broadcasted_iota(jnp.int32, (1, BLOCK), 1)
        scale = jnp.where(point < live_points, unit[0:1, 0:1], 0.0)
        at = pl.ds(start, BLOCK)
        for matrix in range(2):
            pieces = [
                jnp.sum(sums_kept[matrix, cut : cut + TILE, :].T, axis=0, keepdims=True)
                for cut in range(0, BLOCK, TILE)
            ]
            line = jnp.concatenate(pieces, axis=1) * scale
            if slot:
                density[matrix, pl.ds(batch, 1), at] = line
            else:
                density[matrix : matrix + 1, at] = line

    def densities(tiles):
        def block(step, carry):
            value_copy(step).wait()
            reduce(jnp.maximum(step - 1, 0))
            start = pl.multiple_of(step * BLOCK, BLOCK)
            columns = []
            for place in range(tiles):
                lane = pl.multiple_of(table[base + place] * TILE, TILE)
                columns.append(values_in[pl.ds(start, BLOCK), pl.ds(lane, TILE)])
            values = jnp.concatenate(columns, axis=1)
            sums = [None, None]
            for last in range(tiles):
                cols = slice(2 * last * TILE, (2 * last + 2) * TILE)
                down = (last + 1) * TILE
                both = jnp.concatenate(columns[: last + 1] + columns[:last], axis=1)
                got = jnp.dot(
                    both, parts[: (2 * last + 1) * TILE, cols], preferred_element_type=jnp.float32
                )
                column = columns[last].astype(jnp.float32)
                for matrix in range(2):
                    part = got[:, matrix * TILE : (matrix + 1) * TILE] * column
                    sums[matrix] = part if last == 0 else sums[matrix] + part
            for matrix in range(2):
                sums_kept[matrix] = sums[matrix]
            return carry

        lax.fori_loop(0, blocks, block, 0)

    for tiles in range(KT - 2, KT + 1):
        pl.when(count == tiles)(lambda tiles=tiles: densities(tiles))
    reduce(jnp.maximum(blocks - 1, 0))

    density_copy = pltpu.make_async_copy(density, density_out, out_sems.at[0])
    density_copy.start()
    mine = pl.ds(batch, 1)
    x = offsets[0, mine, :]
    y = offsets[1, mine, :]
    z = offsets[2, mine, :]
    weight = weights[mine, :]
    near = lax.rem(atoms[mine, :] - base_atom + 2 * ATOMS, ATOMS)
    squared = x * x + y * y + z * z
    shapes = [
        jnp.ones_like(x), x, y, z, x * y, y * z,
        3.0 * z * z - squared, x * z, x * x - y * y,
    ]
    shapes = jnp.concatenate([weight * shape for shape in shapes], axis=0)
    lane = lax.broadcasted_iota(jnp.int32, (9, TILE), 1)
    degree = lax.broadcasted_iota(jnp.int32, (9, TILE), 0)
    lane = lane - degree * SPAN - 4 * batch
    for matrix in range(2):
        terms = density[matrix, mine, :] if slot else density[matrix : matrix + 1, :]
        terms = terms * shapes
        total = jnp.zeros((9, TILE), jnp.float32)
        for atom in range(8):
            picked = jnp.sum(jnp.where(near == atom, terms, 0.0), axis=1, keepdims=True)
            total = total + jnp.where(lane == atom, picked, 0.0)
        line = jnp.sum(total, axis=0, keepdims=True)
        if slot:
            line = line + before[matrix : matrix + 1, :]
            payload[:, matrix : matrix + 1, :] = jnp.broadcast_to(line[None], (DEVICES, 1, TILE))
        else:
            payload[matrix : matrix + 1, :] = line
    density_copy.wait()


def batch_call(slot, table, rows, carried, unit, offsets, weights, atoms, basis):
    arrays = [table, rows, *carried, unit, offsets, weights, atoms, basis]
    payload = (DEVICES, 2, TILE) if slot else (2, TILE)
    density = (2, 2, PTS) if slot else (2, PTS)
    own_rows = []
    if slot:
        own_rows = [
            pltpu.VMEM((DEVICES * PAIRS, TILE), jnp.int32),
            pltpu.SemaphoreType.DMA((4,)),
        ]

    def body(*refs):
        batch_body(slot, *refs)

    return pl.pallas_call(
        body,
        in_specs=[
            pl.BlockSpec(memory_space=pltpu.SMEM),
            pl.BlockSpec(memory_space=pltpu.HBM if slot else pltpu.VMEM),
            *[pl.BlockSpec(memory_space=pltpu.VMEM) for _ in arrays[2:-1]],
            pl.BlockSpec(memory_space=pltpu.HBM),
        ],
        out_specs=(
            pl.BlockSpec(memory_space=pl.ANY),
            pl.BlockSpec(memory_space=pltpu.VMEM),
        ),
        out_shape=(
            jax.ShapeDtypeStruct(density, jnp.float32),
            pltpu.VMEM(payload, jnp.float32),
        ),
        scratch_shapes=[
            pltpu.VMEM(((2 * KT - 1) * TILE, 2 * KT * TILE), jnp.bfloat16),
            pltpu.VMEM((PTS, KT * TILE), jnp.bfloat16),
            pltpu.VMEM(density, jnp.float32),
            pltpu.VMEM((2, BLOCK, TILE), jnp.float32),
            pltpu.SemaphoreType.DMA((STEPS,)),
            pltpu.SemaphoreType.DMA((1,)),
            *own_rows,
        ],
        compiler_params=pltpu.CompilerParams(vmem_limit_bytes=48 * 1024 * 1024),
        cost_estimate=pl.CostEstimate(
            flops=26_000_000_000, bytes_accessed=10_000_000, transcendentals=0
        ),
        name=f"batch_density_{slot}",
    )(*arrays)


def moment_body(arrived, out):
    lane = lax.broadcasted_iota(jnp.int32, (8, TILE), 1)
    for matrix in range(2):
        totals = [jnp.zeros((8, TILE), jnp.float32) for _ in range(9)]
        for place in range(16):
            part = arrived[pl.ds(2 * place + matrix, 8, stride=32), :]
            for degree in range(9):
                moved = pltpu.roll(part, (8 * place - SPAN * degree) % TILE, 1)
                if place < 15:
                    mine = (lane >= 8 * place) & (lane < 8 * place + SPAN)
                    totals[degree] = totals[degree] + jnp.where(mine, moved, 0.0)
                else:
                    inside = jnp.where(lane >= 8 * place, moved, 0.0)
                    after = pltpu.roll(jnp.where(lane < SPAN - 8, moved, 0.0), 1, 0)
                    totals[degree] = totals[degree] + inside + after
        for degree in range(9):
            for block in range(8):
                out[degree, matrix : matrix + 1, block * TILE : (block + 1) * TILE] = totals[degree][
                    block : block + 1, :
                ]


def moment_table(arrived):
    return pl.pallas_call(
        moment_body,
        out_shape=jax.ShapeDtypeStruct((9, 2, ATOMS), jnp.float32),
        in_specs=[pl.BlockSpec(memory_space=pltpu.VMEM)],
        out_specs=pl.BlockSpec(memory_space=pltpu.VMEM),
        compiler_params=pltpu.CompilerParams(vmem_limit_bytes=8 * 1024 * 1024),
        name="moment_table",
    )(arrived)


def exchange(value):
    return lax.all_to_all(value, ROW_COL, 0, 0, tiled=True)


def exchange_windows(rows):
    return exchange(rows.reshape(DEVICES, PAIRS // 4, 4, TILE)).reshape(DEVICES * PAIRS, TILE)


def local(
    density_first,
    density_second,
    basis,
    tile_list,
    tile_count,
    point_count,
    offsets,
    weights,
    atom_of_point,
):
    rows = spread(tile_list, tile_count, point_count, density_first, density_second)
    rows = exchange(rows.reshape(DEVICES, LINES, TILE)).reshape(DEVICES * LINES, TILE)
    first, coded, starts, unit = windows(rows)
    first = exchange_windows(first)
    rest = exchange_windows(rest_windows(starts, coded))

    table = batch_tables(tile_list, tile_count, point_count)
    flat = basis.reshape(-1, KT * TILE)
    side = (unit, offsets, weights, atom_of_point)
    density_0, payload_0 = batch_call(0, table, first, (), *side, flat)
    density, payload = batch_call(
        1, table, rest, (payload_0, density_0), *side, flat
    )
    moments = moment_table(exchange(payload).reshape(DEVICES * 2, TILE)).swapaxes(0, 1)
    return density, moments


def solution(mesh):
    torus = Mesh(mesh.devices.reshape(4, 4, 4, 2), ("row_0", "row_1", "col_0", "col_1"))
    in_specs = (
        P(ROW, COL),
        P(ROW, COL),
        P(ROW_COL, None, None),
        P(ROW_COL, None),
        P(ROW_COL),
        P(ROW_COL),
        P(None, ROW_COL, None),
        P(ROW_COL, None),
        P(ROW_COL, None),
    )
    out_specs = (P(None, ROW_COL, None), P())
    return jax.shard_map(local, mesh=torus, in_specs=in_specs, out_specs=out_specs, check_vma=False)
```

```python
import jax
import jax.numpy as jnp
from jax import lax
from jax.experimental import pallas as pl
from jax.experimental.pallas import tpu as pltpu
from jax.sharding import Mesh
from jax.sharding import PartitionSpec as P

TILE = 128
KT = 7
NT = 96
PTS = 4096
ATOMS = 1024
N_ROW = 16
N_COL = 8
DEVICES = 128
SPAN = 12
ROW = ("row_0", "row_1")
COL = ("col_0", "col_1")
ROW_COL = ("row_0", "row_1", "col_0", "col_1")

SLOTS = 24
LINES = 28
PAIRS = KT * (KT + 1) // 2
WINDOW = 2 * PAIRS
GROUPS = 4
FRONT = 1152
BACK = 1536
BLOCK = 512
STEPS = PTS // BLOCK
ROUNDER = 12582912.0


def pair_start(last):
    return last * (last + 1) // 2


def spread_body(
    list_in, tiles_in, points_in, first, second, out,
    tiles, lines, tile_list, tile_count, point_count, sems,
):
    my_row = lax.axis_index(ROW)
    my_col = lax.axis_index(COL)
    small = [
        pltpu.make_async_copy(source, target, sems.at[SLOTS + place])
        for place, (source, target) in enumerate(
            ((list_in, tile_list), (tiles_in, tile_count), (points_in, point_count))
        )
    ]
    for copy in small:
        copy.start()
    lead = lax.rem(my_col - my_row + 16, 8)
    base = (my_row - my_col + lead) // 8
    copies = []
    for half in range(2):
        for step in range(6):
            for which, stored in enumerate((first, second)):
                index = which * 12 + half * 6 + step
                column = jnp.clip(2 * step + base - half, 0, 11)
                copy = pltpu.make_async_copy(
                    stored.at[pl.ds(step * TILE, TILE), pl.ds(pl.multiple_of(column * TILE, TILE), TILE)],
                    tiles.at[index],
                    sems.at[index],
                )
                copy.start()
                copies.append((copy, index, half, step))
    largest = jnp.zeros((8, TILE), jnp.float32)
    for copy, index, half, step in copies:
        copy.wait()
        values = tiles[index].astype(jnp.float32)
        column = 2 * step + base - half
        shift = lead - 8 * half
        used = (column >= 0) & (column < 12) & (shift <= 6) & (shift >= -6)
        peak = jnp.max(jnp.abs(values).reshape(16, 8, TILE), axis=0)
        largest = jnp.maximum(largest, jnp.where(used, peak, 0.0))
        if half:
            values = values.T
        lines[pl.ds(index, TILE, stride=SLOTS), :] = values
    for copy in small:
        copy.wait()
    own_start = [least_tile(tile_list, batch) for batch in slot_order(tile_count, point_count)]
    peak = jnp.max(largest)
    line = lax.broadcasted_iota(jnp.int32, (4, TILE), 0)
    extra = jnp.where(
        line == 0,
        own_start[0].astype(jnp.float32),
        jnp.where(line == 1, own_start[1].astype(jnp.float32), peak),
    )

    def pack(group, carry):
        pieces = []
        for dest in range(4):
            at = pl.multiple_of((group * 4 + dest) * SLOTS, 8)
            pieces += [lines[pl.ds(at, SLOTS), :], extra]
        to = pl.multiple_of(group * 4 * LINES, 16)
        out[pl.ds(to, 4 * LINES), :] = jnp.concatenate(pieces, axis=0).astype(jnp.bfloat16)
        return carry

    lax.fori_loop(0, DEVICES // 4, pack, 0, unroll=2)


def spread(tile_list, tile_count, point_count, first, second):
    return pl.pallas_call(
        spread_body,
        out_shape=pltpu.VMEM((DEVICES * LINES, TILE), jnp.bfloat16),
        in_specs=[
            pl.BlockSpec(memory_space=pl.ANY),
            pl.BlockSpec(memory_space=pl.ANY),
            pl.BlockSpec(memory_space=pl.ANY),
            pl.BlockSpec(memory_space=pl.ANY),
            pl.BlockSpec(memory_space=pl.ANY),
        ],
        out_specs=pl.BlockSpec(memory_space=pltpu.VMEM),
        scratch_shapes=[
            pltpu.VMEM((SLOTS, TILE, TILE), jnp.bfloat16),
            pltpu.VMEM((DEVICES * SLOTS, TILE), jnp.float32),
            pltpu.SMEM((2, KT), jnp.int32),
            pltpu.SMEM((2,), jnp.int32),
            pltpu.SMEM((2,), jnp.int32),
            pltpu.SemaphoreType.DMA((SLOTS + 3,)),
        ],
        name="spread_rows",
    )(tile_list, tile_count, point_count, first, second)


def window_body(
    arrived, first_out, coded_to, starts_to, unit_to,
    lines, coded, start_lines, starts, out_first, unit_out, sem, out_sems,
):
    def widen(group, top):
        peak, own = top
        lane = lax.broadcasted_iota(jnp.int32, (4, TILE), 1)
        at = pl.multiple_of(group * 4 * LINES, 16)
        block = arrived[pl.ds(at, 4 * LINES), :].astype(jnp.float32)
        for place in range(4):
            source = group * 4 + place
            to = pl.multiple_of(FRONT + source * SLOTS, 8)
            lines[pl.ds(to, SLOTS), :] = block[place * LINES : place * LINES + SLOTS]
            extra = block[place * LINES + SLOTS : (place + 1) * LINES]
            own = jnp.where(lane == source, extra, own)
            peak = jnp.maximum(peak, extra)
        return peak, own

    zero = jnp.zeros((4, TILE), jnp.float32)
    tops, own = lax.fori_loop(0, DEVICES // 4, widen, (zero, zero), unroll=2)
    start_lines[0:4, :] = own.astype(jnp.int32)
    start_lines[4:8, :] = jnp.zeros((4, TILE), jnp.int32)
    copy = pltpu.make_async_copy(start_lines, starts, sem)
    copy.start()
    starts_copy = pltpu.make_async_copy(start_lines, starts_to, out_sems.at[2])
    starts_copy.start()
    peak = jnp.broadcast_to(tops[2:3, :], (8, TILE))
    scale = jnp.full((8, TILE), 2.0**21, jnp.float32)
    unit = jnp.full((8, TILE), 2.0**-21, jnp.float32)
    for step in range(1, 64):
        small = peak < 2.0 ** (-7 - step)
        scale = jnp.where(small, 2.0 ** (21 + step), scale)
        unit = jnp.where(small, 2.0 ** (-21 - step), unit)
    unit_out[...] = unit
    unit_copy = pltpu.make_async_copy(unit_out, unit_to, out_sems.at[0])
    unit_copy.start()

    order = lax.broadcasted_iota(jnp.int32, (8, TILE), 0)

    def line_of(row, col, which, half, step):
        return FRONT + (row * N_COL + col) * SLOTS + which * 12 + half * 6 + step

    def eight(start):
        return lines[pl.ds(start, 8, stride=(N_COL + 1) * SLOTS), :]

    for apart in range(KT):
        for group in range(NT // 8):
            words = []
            for which in range(2):
                odd = group % 2
                step = group // 2
                if odd or apart == 0:
                    total = eight(line_of(8 * odd - apart, 0, which, 0, step))
                else:
                    total = eight(line_of(-apart, 0, which, 0, step))
                    if step > 0:
                        before = eight(line_of(16 - apart, 0, which, 0, step - 1))
                        total = jnp.where(order < apart, before, total)
                if apart > 0:
                    after = eight(line_of(8 * odd, -apart, which, 1, step))
                    wrapped = eight(line_of(8 * odd, 8 - apart, which, 1, step))
                    total = total + jnp.where(order < apart, wrapped, after)
                total = total * scale
                words.append(((total + ROUNDER) - ROUNDER).astype(jnp.int32))
            word = (words[0] << 16) | (words[1] & 0xFFFF)
            coded[pl.ds(group * 64 + apart, 8, stride=8), :] = word

    coded_copy = pltpu.make_async_copy(coded, coded_to, out_sems.at[1])
    coded_copy.start()
    copy.wait()
    copies = fill_windows(0, starts, coded, out_first, first_out, out_sems)
    for copy in [unit_copy, starts_copy, coded_copy, *copies]:
        copy.wait()


def fill_windows(slot, starts, coded, filled, out, sems):
    def fill(pair, carry):
        for half in range(2):
            start = starts[slot, 2 * pair + half]
            for last in range(KT):
                words = coded[pl.ds(pl.multiple_of((start + last) * 8, 8), 8), :]
                low = half * PAIRS + pair_start(last)
                filled[pair, low : low + last + 1, :] = words[: last + 1]
        return carry

    copies = []
    group = DEVICES // 2 // GROUPS
    for part in range(GROUPS):
        lax.fori_loop(part * group, (part + 1) * group, fill, 0, unroll=2)
        span = pl.ds(part * group, group)
        copy = pltpu.make_async_copy(filled.at[span], out.at[span], sems.at[3 + part])
        copy.start()
        copies.append(copy)
    return copies


def windows(arrived):
    return pl.pallas_call(
        window_body,
        out_shape=(
            pltpu.HBM((DEVICES // 2, WINDOW, TILE), jnp.int32),
            pltpu.HBM((NT * 8, TILE), jnp.int32),
            pltpu.HBM((8, TILE), jnp.int32),
            pltpu.HBM((8, TILE), jnp.float32),
        ),
        in_specs=[pl.BlockSpec(memory_space=pltpu.VMEM)],
        out_specs=tuple(pl.BlockSpec(memory_space=pl.ANY) for _ in range(4)),
        scratch_shapes=[
            pltpu.VMEM((FRONT + DEVICES * SLOTS + BACK, TILE), jnp.float32),
            pltpu.VMEM((NT * 8, TILE), jnp.int32),
            pltpu.VMEM((8, TILE), jnp.int32),
            pltpu.SMEM((8, TILE), jnp.int32),
            pltpu.VMEM((DEVICES // 2, WINDOW, TILE), jnp.int32),
            pltpu.VMEM((8, TILE), jnp.float32),
            pltpu.SemaphoreType.DMA,
            pltpu.SemaphoreType.DMA((3 + GROUPS,)),
        ],
        compiler_params=pltpu.CompilerParams(vmem_limit_bytes=24 * 1024 * 1024),
        name="pick_windows",
    )(arrived)


def rest_body(starts, coded, out, filled, sems):
    for copy in fill_windows(1, starts, coded, filled, out, sems):
        copy.wait()


def rest_windows(starts, coded):
    return pl.pallas_call(
        rest_body,
        out_shape=jax.ShapeDtypeStruct((DEVICES // 2, WINDOW, TILE), jnp.int32),
        in_specs=[
            pl.BlockSpec(memory_space=pltpu.SMEM),
            pl.BlockSpec(memory_space=pltpu.VMEM),
        ],
        out_specs=pl.BlockSpec(memory_space=pl.ANY),
        scratch_shapes=[
            pltpu.VMEM((DEVICES // 2, WINDOW, TILE), jnp.int32),
            pltpu.SemaphoreType.DMA((3 + GROUPS,)),
        ],
        name="pick_rest",
    )(starts, coded)


def slot_order(tile_count, point_count):
    work = []
    for batch in range(2):
        count = tile_count[batch]
        passes = jnp.where(count >= KT, 28, jnp.where(count == KT - 1, 21, 15))
        work.append(passes * point_count[batch])
    swap = (work[1] > work[0]).astype(jnp.int32)
    return swap, 1 - swap


def least_tile(tile_list, batch):
    least = tile_list[batch, 0]
    for place in range(1, KT):
        least = jnp.minimum(least, tile_list[batch, place])
    return least


COUNT = 7
POINTS = 8
ATOM = 9
BATCH = 10
LINE = 11
ENTRIES = 40


def table_body(tile_list, tile_count, point_count, table, column_of, order_of):
    device = lax.axis_index(ROW) * N_COL + lax.axis_index(COL)
    for slot, batch in enumerate(slot_order(tile_count, point_count)):
        base = slot * ENTRIES
        start = least_tile(tile_list, batch)
        count = jnp.minimum(tile_count[batch], KT)
        for place in range(KT):
            column_of[tile_list[batch, place] - start] = place
        live_end = 0
        dead_end = count
        for rank in range(KT):
            place = column_of[rank]
            live = (place < count).astype(jnp.int32)
            to = jnp.where(live == 1, live_end, dead_end)
            table[base + to] = place
            order_of[to] = rank
            live_end = live_end + live
            dead_end = dead_end + 1 - live
        table[base + COUNT] = count
        table[base + POINTS] = point_count[batch]
        table[base + ATOM] = lax.rem((2 * device + batch) * 4, ATOMS)
        table[base + BATCH] = batch
        for last in range(KT):
            high = order_of[last]
            for first in range(last + 1):
                low = order_of[first]
                line = high * (high + 1) // 2 + high - low
                table[base + LINE + pair_start(last) + first] = jnp.where(last < count, line, 0)


def batch_tables(tile_list, tile_count, point_count):
    return pl.pallas_call(
        table_body,
        out_shape=jax.ShapeDtypeStruct((2 * ENTRIES,), jnp.int32),
        in_specs=[pl.BlockSpec(memory_space=pltpu.SMEM) for _ in range(3)],
        out_specs=pl.BlockSpec(memory_space=pltpu.SMEM),
        scratch_shapes=[pltpu.SMEM((8,), jnp.int32), pltpu.SMEM((8,), jnp.int32)],
        name="batch_tables",
    )(tile_list, tile_count, point_count)


def batch_body(slot, *refs):
    table, rows = refs[:2]
    refs = refs[2:]
    if slot:
        before, earlier = refs[:2]
        refs = refs[2:]
    unit, offsets, weights, atoms, basis, density_out, payload = refs[:7]
    parts, values_in, density, sums_kept = refs[7:11]
    value_sems, out_sems = refs[11:13]
    base = slot * ENTRIES
    if slot:
        rows_here, row_sems = refs[13:]
        row_copies = []
        for group in range(4):
            span = pl.ds(group * (DEVICES * PAIRS // 4), DEVICES * PAIRS // 4)
            row_copies.append(
                pltpu.make_async_copy(rows.at[span], rows_here.at[span], row_sems.at[group])
            )
        for copy in row_copies:
            copy.start()
        rows = rows_here
    count = table[base + COUNT]
    live_points = table[base + POINTS]
    base_atom = table[base + ATOM]
    batch = table[base + BATCH]

    def value_copy(step):
        return pltpu.make_async_copy(
            basis.at[pl.ds(pl.multiple_of(batch * PTS + step * BLOCK, BLOCK), BLOCK), :],
            values_in.at[pl.ds(pl.multiple_of(step * BLOCK, BLOCK), BLOCK), :],
            value_sems.at[step],
        )

    for step in range(STEPS):
        pl.when(step * BLOCK < live_points)(lambda step=step: value_copy(step).start())
    if not slot:
        density[...] = jnp.zeros((2, PTS), jnp.float32)

    def unpack(last, part, size):
        for first in range(last + 1):
            start = table[base + LINE + pair_start(last) + first] + part * size * PAIRS
            words = rows[pl.ds(start, size, stride=PAIRS), :]
            down = slice(first * TILE + part * size, first * TILE + (part + 1) * size)
            low = (last + 1 + first) * TILE + part * size
            for matrix in range(2):
                value = words >> 16 if matrix == 0 else (words << 16) >> 16
                value = value.astype(jnp.float32)
                top = value.astype(jnp.bfloat16)
                at = (2 * last + matrix) * TILE
                parts[down, at : at + TILE] = top
                if first < last:
                    bottom = (value - top.astype(jnp.float32)).astype(jnp.bfloat16)
                    parts[low : low + size, at : at + TILE] = bottom

    pieces = 4 if slot else 1
    for part in range(pieces):
        if slot:
            row_copies[part].wait()
        size = TILE // pieces
        for last in range(KT - 2):
            unpack(last, part, size)
        for last in range(KT - 2, KT):
            pl.when(count > last)(lambda last=last: unpack(last, part, size))
    if slot:
        which = lax.broadcasted_iota(jnp.int32, (2, PTS), 0)
        for matrix in range(2):
            other = jnp.broadcast_to(earlier[matrix : matrix + 1, :], (2, PTS))
            density[matrix] = jnp.where(which == batch, 0.0, other)

    blocks = (live_points + BLOCK - 1) // BLOCK

    def reduce(step):
        start = pl.multiple_of(step * BLOCK, BLOCK)
        point = start + lax.broadcasted_iota(jnp.int32, (1, BLOCK), 1)
        scale = jnp.where(point < live_points, unit[0:1, 0:1], 0.0)
        at = pl.ds(start, BLOCK)
        for matrix in range(2):
            pieces = [
                jnp.sum(sums_kept[matrix, cut : cut + TILE, :].T, axis=0, keepdims=True)
                for cut in range(0, BLOCK, TILE)
            ]
            line = jnp.concatenate(pieces, axis=1) * scale
            if slot:
                density[matrix, pl.ds(batch, 1), at] = line
            else:
                density[matrix : matrix + 1, at] = line

    def densities(tiles):
        def block(step, carry):
            value_copy(step).wait()
            reduce(jnp.maximum(step - 1, 0))
            start = pl.multiple_of(step * BLOCK, BLOCK)
            columns = []
            for place in range(tiles):
                lane = pl.multiple_of(table[base + place] * TILE, TILE)
                columns.append(values_in[pl.ds(start, BLOCK), pl.ds(lane, TILE)])
            values = jnp.concatenate(columns, axis=1)
            sums = [None, None]
            for last in range(tiles):
                cols = slice(2 * last * TILE, (2 * last + 2) * TILE)
                down = (last + 1) * TILE
                both = jnp.concatenate(columns[: last + 1] + columns[:last], axis=1)
                got = jnp.dot(
                    both, parts[: (2 * last + 1) * TILE, cols], preferred_element_type=jnp.float32
                )
                column = columns[last].astype(jnp.float32)
                for matrix in range(2):
                    part = got[:, matrix * TILE : (matrix + 1) * TILE] * column
                    sums[matrix] = part if last == 0 else sums[matrix] + part
            for matrix in range(2):
                sums_kept[matrix] = sums[matrix]
            return carry

        lax.fori_loop(0, blocks, block, 0)

    for tiles in range(KT - 2, KT + 1):
        pl.when(count == tiles)(lambda tiles=tiles: densities(tiles))
    reduce(jnp.maximum(blocks - 1, 0))

    density_copy = pltpu.make_async_copy(density, density_out, out_sems.at[0])
    density_copy.start()
    mine = pl.ds(batch, 1)
    x = offsets[0, mine, :]
    y = offsets[1, mine, :]
    z = offsets[2, mine, :]
    weight = weights[mine, :]
    near = lax.rem(atoms[mine, :] - base_atom + 2 * ATOMS, ATOMS)
    squared = x * x + y * y + z * z
    shapes = [
        jnp.ones_like(x), x, y, z, x * y, y * z,
        3.0 * z * z - squared, x * z, x * x - y * y,
    ]
    shapes = jnp.concatenate([weight * shape for shape in shapes], axis=0)
    lane = lax.broadcasted_iota(jnp.int32, (9, TILE), 1)
    degree = lax.broadcasted_iota(jnp.int32, (9, TILE), 0)
    lane = lane - degree * SPAN - 4 * batch
    for matrix in range(2):
        terms = density[matrix, mine, :] if slot else density[matrix : matrix + 1, :]
        terms = terms * shapes
        total = jnp.zeros((9, TILE), jnp.float32)
        for atom in range(8):
            picked = jnp.sum(jnp.where(near == atom, terms, 0.0), axis=1, keepdims=True)
            total = total + jnp.where(lane == atom, picked, 0.0)
        line = jnp.sum(total, axis=0, keepdims=True)
        if slot:
            line = line + before[matrix : matrix + 1, :]
            payload[:, matrix : matrix + 1, :] = jnp.broadcast_to(line[None], (DEVICES, 1, TILE))
        else:
            payload[matrix : matrix + 1, :] = line
    density_copy.wait()


def batch_call(slot, table, rows, carried, unit, offsets, weights, atoms, basis):
    arrays = [table, rows, *carried, unit, offsets, weights, atoms, basis]
    payload = (DEVICES, 2, TILE) if slot else (2, TILE)
    density = (2, 2, PTS) if slot else (2, PTS)
    own_rows = []
    if slot:
        own_rows = [
            pltpu.VMEM((DEVICES * PAIRS, TILE), jnp.int32),
            pltpu.SemaphoreType.DMA((4,)),
        ]

    def body(*refs):
        batch_body(slot, *refs)

    return pl.pallas_call(
        body,
        in_specs=[
            pl.BlockSpec(memory_space=pltpu.SMEM),
            pl.BlockSpec(memory_space=pltpu.HBM if slot else pltpu.VMEM),
            *[pl.BlockSpec(memory_space=pltpu.VMEM) for _ in arrays[2:-1]],
            pl.BlockSpec(memory_space=pltpu.HBM),
        ],
        out_specs=(
            pl.BlockSpec(memory_space=pl.ANY),
            pl.BlockSpec(memory_space=pltpu.VMEM),
        ),
        out_shape=(
            jax.ShapeDtypeStruct(density, jnp.float32),
            pltpu.VMEM(payload, jnp.float32),
        ),
        scratch_shapes=[
            pltpu.VMEM(((2 * KT - 1) * TILE, 2 * KT * TILE), jnp.bfloat16),
            pltpu.VMEM((PTS, KT * TILE), jnp.bfloat16),
            pltpu.VMEM(density, jnp.float32),
            pltpu.VMEM((2, BLOCK, TILE), jnp.float32),
            pltpu.SemaphoreType.DMA((STEPS,)),
            pltpu.SemaphoreType.DMA((1,)),
            *own_rows,
        ],
        compiler_params=pltpu.CompilerParams(vmem_limit_bytes=48 * 1024 * 1024),
        cost_estimate=pl.CostEstimate(
            flops=26_000_000_000, bytes_accessed=10_000_000, transcendentals=0
        ),
        name=f"batch_density_{slot}",
    )(*arrays)


def moment_body(arrived, out):
    lane = lax.broadcasted_iota(jnp.int32, (8, TILE), 1)
    for matrix in range(2):
        totals = [jnp.zeros((8, TILE), jnp.float32) for _ in range(9)]
        for place in range(16):
            part = arrived[pl.ds(2 * place + matrix, 8, stride=32), :]
            for degree in range(9):
                moved = pltpu.roll(part, (8 * place - SPAN * degree) % TILE, 1)
                if place < 15:
                    mine = (lane >= 8 * place) & (lane < 8 * place + SPAN)
                    totals[degree] = totals[degree] + jnp.where(mine, moved, 0.0)
                else:
                    inside = jnp.where(lane >= 8 * place, moved, 0.0)
                    after = pltpu.roll(jnp.where(lane < SPAN - 8, moved, 0.0), 1, 0)
                    totals[degree] = totals[degree] + inside + after
        for degree in range(9):
            for block in range(8):
                out[degree, matrix : matrix + 1, block * TILE : (block + 1) * TILE] = totals[degree][
                    block : block + 1, :
                ]


def moment_table(arrived):
    return pl.pallas_call(
        moment_body,
        out_shape=jax.ShapeDtypeStruct((9, 2, ATOMS), jnp.float32),
        in_specs=[pl.BlockSpec(memory_space=pltpu.VMEM)],
        out_specs=pl.BlockSpec(memory_space=pltpu.VMEM),
        compiler_params=pltpu.CompilerParams(vmem_limit_bytes=8 * 1024 * 1024),
        name="moment_table",
    )(arrived)


def exchange(value):
    return lax.all_to_all(value, ROW_COL, 0, 0, tiled=True)


def exchange_lines(rows):
    return exchange(rows.reshape(DEVICES, -1, 4, TILE)).reshape(-1, TILE)


def local(
    density_first,
    density_second,
    basis,
    tile_list,
    tile_count,
    point_count,
    offsets,
    weights,
    atom_of_point,
):
    rows = spread(tile_list, tile_count, point_count, density_first, density_second)
    rows = exchange_lines(rows)
    first, coded, starts, unit = windows(rows)
    first = exchange_lines(first)
    rest = exchange_lines(rest_windows(starts, coded))

    table = batch_tables(tile_list, tile_count, point_count)
    flat = basis.reshape(-1, KT * TILE)
    side = (unit, offsets, weights, atom_of_point)
    density_0, payload_0 = batch_call(0, table, first, (), *side, flat)
    density, payload = batch_call(
        1, table, rest, (payload_0, density_0), *side, flat
    )
    moments = moment_table(exchange(payload).reshape(DEVICES * 2, TILE)).swapaxes(0, 1)
    return density, moments


def solution(mesh):
    torus = Mesh(mesh.devices.reshape(4, 4, 4, 2), ("row_0", "row_1", "col_0", "col_1"))
    in_specs = (
        P(ROW, COL),
        P(ROW, COL),
        P(ROW_COL, None, None),
        P(ROW_COL, None),
        P(ROW_COL),
        P(ROW_COL),
        P(None, ROW_COL, None),
        P(ROW_COL, None),
        P(ROW_COL, None),
    )
    out_specs = (P(None, ROW_COL, None), P())
    return jax.shard_map(local, mesh=torus, in_specs=in_specs, out_specs=out_specs, check_vma=False)
```

```python
import jax
import jax.numpy as jnp
from jax import lax
from jax.experimental import pallas as pl
from jax.experimental.pallas import tpu as pltpu
from jax.sharding import Mesh
from jax.sharding import PartitionSpec as P

TILE = 128
KT = 7
NT = 96
PTS = 4096
ATOMS = 1024
N_ROW = 16
N_COL = 8
DEVICES = 128
SPAN = 12
ROW = ("row_0", "row_1")
COL = ("col_0", "col_1")
ROW_COL = ("row_0", "row_1", "col_0", "col_1")

SLOTS = 24
LINES = 28
PAIRS = KT * (KT + 1) // 2
WINDOW = 2 * PAIRS
GROUPS = 4
FRONT = 1152
BACK = 1536
BLOCK = 512
STEPS = PTS // BLOCK
ROUNDER = 12582912.0


def pair_start(last):
    return last * (last + 1) // 2


def spread_body(
    list_in, tiles_in, points_in, first, second, out,
    tiles, lines, tile_list, tile_count, point_count, sems,
):
    my_row = lax.axis_index(ROW)
    my_col = lax.axis_index(COL)
    small = [
        pltpu.make_async_copy(source, target, sems.at[SLOTS + place])
        for place, (source, target) in enumerate(
            ((list_in, tile_list), (tiles_in, tile_count), (points_in, point_count))
        )
    ]
    for copy in small:
        copy.start()
    lead = lax.rem(my_col - my_row + 16, 8)
    base = (my_row - my_col + lead) // 8
    copies = []
    for half in range(2):
        for step in range(6):
            for which, stored in enumerate((first, second)):
                index = which * 12 + half * 6 + step
                column = jnp.clip(2 * step + base - half, 0, 11)
                copy = pltpu.make_async_copy(
                    stored.at[pl.ds(step * TILE, TILE), pl.ds(pl.multiple_of(column * TILE, TILE), TILE)],
                    tiles.at[index],
                    sems.at[index],
                )
                copy.start()
                copies.append((copy, index, half, step))
    largest = jnp.zeros((8, TILE), jnp.float32)
    for copy, index, half, step in copies:
        copy.wait()
        values = tiles[index].astype(jnp.float32)
        column = 2 * step + base - half
        shift = lead - 8 * half
        used = (column >= 0) & (column < 12) & (shift <= 6) & (shift >= -6)
        peak = jnp.max(jnp.abs(values).reshape(16, 8, TILE), axis=0)
        largest = jnp.maximum(largest, jnp.where(used, peak, 0.0))
        if half:
            values = values.T
        lines[pl.ds(index, TILE, stride=SLOTS), :] = values
    for copy in small:
        copy.wait()
    own_start = [least_tile(tile_list, batch) for batch in slot_order(tile_count, point_count)]
    peak = jnp.max(largest)
    line = lax.broadcasted_iota(jnp.int32, (4, TILE), 0)
    extra = jnp.where(
        line == 0,
        own_start[0].astype(jnp.float32),
        jnp.where(line == 1, own_start[1].astype(jnp.float32), peak),
    )

    def pack(group, carry):
        pieces = []
        for dest in range(4):
            at = pl.multiple_of((group * 4 + dest) * SLOTS, 8)
            pieces += [lines[pl.ds(at, SLOTS), :], extra]
        to = pl.multiple_of(group * 4 * LINES, 16)
        out[pl.ds(to, 4 * LINES), :] = jnp.concatenate(pieces, axis=0).astype(jnp.bfloat16)
        return carry

    lax.fori_loop(0, DEVICES // 4, pack, 0, unroll=2)


def spread(tile_list, tile_count, point_count, first, second):
    return pl.pallas_call(
        spread_body,
        out_shape=pltpu.VMEM((DEVICES * LINES, TILE), jnp.bfloat16),
        in_specs=[
            pl.BlockSpec(memory_space=pl.ANY),
            pl.BlockSpec(memory_space=pl.ANY),
            pl.BlockSpec(memory_space=pl.ANY),
            pl.BlockSpec(memory_space=pl.ANY),
            pl.BlockSpec(memory_space=pl.ANY),
        ],
        out_specs=pl.BlockSpec(memory_space=pltpu.VMEM),
        scratch_shapes=[
            pltpu.VMEM((SLOTS, TILE, TILE), jnp.bfloat16),
            pltpu.VMEM((DEVICES * SLOTS, TILE), jnp.float32),
            pltpu.SMEM((2, KT), jnp.int32),
            pltpu.SMEM((2,), jnp.int32),
            pltpu.SMEM((2,), jnp.int32),
            pltpu.SemaphoreType.DMA((SLOTS + 3,)),
        ],
        name="spread_rows",
    )(tile_list, tile_count, point_count, first, second)


def window_body(
    arrived, first_out, coded_to, starts_to, unit_to,
    lines, coded, start_lines, starts, out_first, unit_out, sem, out_sems,
):
    def widen(group, top):
        peak, own = top
        lane = lax.broadcasted_iota(jnp.int32, (4, TILE), 1)
        at = pl.multiple_of(group * 4 * LINES, 16)
        block = arrived[pl.ds(at, 4 * LINES), :].astype(jnp.float32)
        for place in range(4):
            source = group * 4 + place
            to = pl.multiple_of(FRONT + source * SLOTS, 8)
            lines[pl.ds(to, SLOTS), :] = block[place * LINES : place * LINES + SLOTS]
            extra = block[place * LINES + SLOTS : (place + 1) * LINES]
            own = jnp.where(lane == source, extra, own)
            peak = jnp.maximum(peak, extra)
        return peak, own

    zero = jnp.zeros((4, TILE), jnp.float32)
    tops, own = lax.fori_loop(0, DEVICES // 4, widen, (zero, zero), unroll=2)
    start_lines[0:4, :] = own.astype(jnp.int32)
    start_lines[4:8, :] = jnp.zeros((4, TILE), jnp.int32)
    copy = pltpu.make_async_copy(start_lines, starts, sem)
    copy.start()
    starts_copy = pltpu.make_async_copy(start_lines, starts_to, out_sems.at[2])
    starts_copy.start()
    peak = jnp.broadcast_to(tops[2:3, :], (8, TILE))
    scale = jnp.full((8, TILE), 2.0**21, jnp.float32)
    unit = jnp.full((8, TILE), 2.0**-21, jnp.float32)
    for step in range(1, 64):
        small = peak < 2.0 ** (-7 - step)
        scale = jnp.where(small, 2.0 ** (21 + step), scale)
        unit = jnp.where(small, 2.0 ** (-21 - step), unit)
    unit_out[...] = unit
    unit_copy = pltpu.make_async_copy(unit_out, unit_to, out_sems.at[0])
    unit_copy.start()

    order = lax.broadcasted_iota(jnp.int32, (8, TILE), 0)

    def line_of(row, col, which, half, step):
        return FRONT + (row * N_COL + col) * SLOTS + which * 12 + half * 6 + step

    def eight(start):
        return lines[pl.ds(start, 8, stride=(N_COL + 1) * SLOTS), :]

    for apart in range(KT):
        for group in range(NT // 8):
            words = []
            for which in range(2):
                odd = group % 2
                step = group // 2
                if odd or apart == 0:
                    total = eight(line_of(8 * odd - apart, 0, which, 0, step))
                else:
                    total = eight(line_of(-apart, 0, which, 0, step))
                    if step > 0:
                        before = eight(line_of(16 - apart, 0, which, 0, step - 1))
                        total = jnp.where(order < apart, before, total)
                if apart > 0:
                    after = eight(line_of(8 * odd, -apart, which, 1, step))
                    wrapped = eight(line_of(8 * odd, 8 - apart, which, 1, step))
                    total = total + jnp.where(order < apart, wrapped, after)
                total = total * scale
                words.append(((total + ROUNDER) - ROUNDER).astype(jnp.int32))
            word = (words[0] << 16) | (words[1] & 0xFFFF)
            coded[pl.ds(group * 64 + apart, 8, stride=8), :] = word

    coded_copy = pltpu.make_async_copy(coded, coded_to, out_sems.at[1])
    coded_copy.start()
    copy.wait()
    copies = fill_windows(0, starts, coded, out_first, first_out, out_sems)
    for copy in [unit_copy, starts_copy, coded_copy, *copies]:
        copy.wait()


def fill_windows(slot, starts, coded, filled, out, sems):
    def fill(pair, carry):
        for half in range(2):
            start = starts[slot, 2 * pair + half]
            for last in range(KT):
                words = coded[pl.ds(pl.multiple_of((start + last) * 8, 8), 8), :]
                low = half * PAIRS + pair_start(last)
                filled[pair, low : low + last + 1, :] = words[: last + 1]
        return carry

    copies = []
    group = DEVICES // 2 // GROUPS
    for part in range(GROUPS):
        lax.fori_loop(part * group, (part + 1) * group, fill, 0, unroll=2)
        span = pl.ds(part * group, group)
        copy = pltpu.make_async_copy(filled.at[span], out.at[span], sems.at[3 + part])
        copy.start()
        copies.append(copy)
    return copies


def windows(arrived):
    return pl.pallas_call(
        window_body,
        out_shape=(
            pltpu.HBM((DEVICES // 2, WINDOW, TILE), jnp.int32),
            pltpu.HBM((NT * 8, TILE), jnp.int32),
            pltpu.HBM((8, TILE), jnp.int32),
            pltpu.HBM((8, TILE), jnp.float32),
        ),
        in_specs=[pl.BlockSpec(memory_space=pltpu.VMEM)],
        out_specs=tuple(pl.BlockSpec(memory_space=pl.ANY) for _ in range(4)),
        scratch_shapes=[
            pltpu.VMEM((FRONT + DEVICES * SLOTS + BACK, TILE), jnp.float32),
            pltpu.VMEM((NT * 8, TILE), jnp.int32),
            pltpu.VMEM((8, TILE), jnp.int32),
            pltpu.SMEM((8, TILE), jnp.int32),
            pltpu.VMEM((DEVICES // 2, WINDOW, TILE), jnp.int32),
            pltpu.VMEM((8, TILE), jnp.float32),
            pltpu.SemaphoreType.DMA,
            pltpu.SemaphoreType.DMA((3 + GROUPS,)),
        ],
        compiler_params=pltpu.CompilerParams(vmem_limit_bytes=24 * 1024 * 1024),
        name="pick_windows",
    )(arrived)


def rest_body(starts, coded, out, filled, sems):
    for copy in fill_windows(1, starts, coded, filled, out, sems):
        copy.wait()


def rest_windows(starts, coded):
    return pl.pallas_call(
        rest_body,
        out_shape=jax.ShapeDtypeStruct((DEVICES // 2, WINDOW, TILE), jnp.int32),
        in_specs=[
            pl.BlockSpec(memory_space=pltpu.SMEM),
            pl.BlockSpec(memory_space=pltpu.VMEM),
        ],
        out_specs=pl.BlockSpec(memory_space=pl.ANY),
        scratch_shapes=[
            pltpu.VMEM((DEVICES // 2, WINDOW, TILE), jnp.int32),
            pltpu.SemaphoreType.DMA((3 + GROUPS,)),
        ],
        name="pick_rest",
    )(starts, coded)


def slot_order(tile_count, point_count):
    work = []
    for batch in range(2):
        count = tile_count[batch]
        passes = jnp.where(count >= KT, 28, jnp.where(count == KT - 1, 21, 15))
        work.append(passes * point_count[batch])
    swap = (work[1] > work[0]).astype(jnp.int32)
    return swap, 1 - swap


def least_tile(tile_list, batch):
    least = tile_list[batch, 0]
    for place in range(1, KT):
        least = jnp.minimum(least, tile_list[batch, place])
    return least


COUNT = 7
POINTS = 8
ATOM = 9
BATCH = 10
LINE = 11
ENTRIES = 40


def table_body(tile_list, tile_count, point_count, table, column_of, order_of):
    device = lax.axis_index(ROW) * N_COL + lax.axis_index(COL)
    for slot, batch in enumerate(slot_order(tile_count, point_count)):
        base = slot * ENTRIES
        start = least_tile(tile_list, batch)
        count = jnp.minimum(tile_count[batch], KT)
        for place in range(KT):
            column_of[tile_list[batch, place] - start] = place
        live_end = 0
        dead_end = count
        for rank in range(KT):
            place = column_of[rank]
            live = (place < count).astype(jnp.int32)
            to = jnp.where(live == 1, live_end, dead_end)
            table[base + to] = place
            order_of[to] = rank
            live_end = live_end + live
            dead_end = dead_end + 1 - live
        table[base + COUNT] = count
        table[base + POINTS] = point_count[batch]
        table[base + ATOM] = lax.rem((2 * device + batch) * 4, ATOMS)
        table[base + BATCH] = batch
        for last in range(KT):
            high = order_of[last]
            for first in range(last + 1):
                low = order_of[first]
                line = high * (high + 1) // 2 + high - low
                table[base + LINE + pair_start(last) + first] = jnp.where(last < count, line, 0)


def batch_tables(tile_list, tile_count, point_count):
    return pl.pallas_call(
        table_body,
        out_shape=jax.ShapeDtypeStruct((2 * ENTRIES,), jnp.int32),
        in_specs=[pl.BlockSpec(memory_space=pltpu.SMEM) for _ in range(3)],
        out_specs=pl.BlockSpec(memory_space=pltpu.SMEM),
        scratch_shapes=[pltpu.SMEM((8,), jnp.int32), pltpu.SMEM((8,), jnp.int32)],
        name="batch_tables",
    )(tile_list, tile_count, point_count)


def batch_body(slot, *refs):
    table, rows = refs[:2]
    refs = refs[2:]
    if slot:
        before, earlier = refs[:2]
        refs = refs[2:]
    unit, offsets, weights, atoms, basis, density_out, payload = refs[:7]
    parts, values_in, density, sums_kept, atom_sums = refs[7:12]
    value_sems, out_sems = refs[12:14]
    base = slot * ENTRIES
    if slot:
        rows_here, row_sems = refs[14:]
        row_copies = []
        for group in range(4):
            span = pl.ds(group * (DEVICES * PAIRS // 4), DEVICES * PAIRS // 4)
            row_copies.append(
                pltpu.make_async_copy(rows.at[span], rows_here.at[span], row_sems.at[group])
            )
        for copy in row_copies:
            copy.start()
        rows = rows_here
    count = table[base + COUNT]
    live_points = table[base + POINTS]
    base_atom = table[base + ATOM]
    batch = table[base + BATCH]

    def value_copy(step):
        return pltpu.make_async_copy(
            basis.at[pl.ds(pl.multiple_of(batch * PTS + step * BLOCK, BLOCK), BLOCK), :],
            values_in.at[pl.ds(pl.multiple_of(step * BLOCK, BLOCK), BLOCK), :],
            value_sems.at[step],
        )

    for step in range(STEPS):
        pl.when(step * BLOCK < live_points)(lambda step=step: value_copy(step).start())
    if not slot:
        density[...] = jnp.zeros((2, PTS), jnp.float32)

    def unpack(last, part, size):
        for first in range(last + 1):
            start = table[base + LINE + pair_start(last) + first] + part * size * PAIRS
            words = rows[pl.ds(start, size, stride=PAIRS), :]
            down = slice(first * TILE + part * size, first * TILE + (part + 1) * size)
            low = (last + 1 + first) * TILE + part * size
            for matrix in range(2):
                value = words >> 16 if matrix == 0 else (words << 16) >> 16
                value = value.astype(jnp.float32)
                top = value.astype(jnp.bfloat16)
                at = (2 * last + matrix) * TILE
                parts[down, at : at + TILE] = top
                if first < last:
                    bottom = (value - top.astype(jnp.float32)).astype(jnp.bfloat16)
                    parts[low : low + size, at : at + TILE] = bottom

    atom_sums[...] = jnp.zeros((16, 16, TILE), jnp.float32)
    pieces = 4 if slot else 1
    for part in range(pieces):
        if slot:
            row_copies[part].wait()
        size = TILE // pieces
        for last in range(KT - 2):
            unpack(last, part, size)
        for last in range(KT - 2, KT):
            pl.when(count > last)(lambda last=last: unpack(last, part, size))
    if slot:
        which = lax.broadcasted_iota(jnp.int32, (2, PTS), 0)
        for matrix in range(2):
            other = jnp.broadcast_to(earlier[matrix : matrix + 1, :], (2, PTS))
            density[matrix] = jnp.where(which == batch, 0.0, other)

    blocks = (live_points + BLOCK - 1) // BLOCK

    def reduce(step, valid):
        start = pl.multiple_of(step * BLOCK, BLOCK)
        point = start + lax.broadcasted_iota(jnp.int32, (1, BLOCK), 1)
        scale = jnp.where(point < live_points, unit[0:1, 0:1], 0.0)
        at = pl.ds(start, BLOCK)
        mine = pl.ds(batch, 1)
        x = offsets[0, mine, at]
        y = offsets[1, mine, at]
        z = offsets[2, mine, at]
        weight = weights[mine, at]
        near = lax.rem(atoms[mine, at] - base_atom + 2 * ATOMS, ATOMS)
        near = jnp.where(valid, near, -1)
        squared = x * x + y * y + z * z
        shapes = [
            jnp.ones_like(x), x, y, z, x * y, y * z,
            3.0 * z * z - squared, x * z, x * x - y * y,
        ]
        shapes = jnp.concatenate([weight * shape for shape in shapes], axis=0)
        for matrix in range(2):
            pieces = [
                jnp.sum(sums_kept[matrix, cut : cut + TILE, :].T, axis=0, keepdims=True)
                for cut in range(0, BLOCK, TILE)
            ]
            line = jnp.concatenate(pieces, axis=1) * scale
            if slot:
                density[matrix, pl.ds(batch, 1), at] = line
            else:
                density[matrix : matrix + 1, at] = line
            terms = line * shapes
            for atom in range(8):
                picked = jnp.where(near == atom, terms, 0.0)
                total = picked[:, :TILE]
                for cut in range(TILE, BLOCK, TILE):
                    total = total + picked[:, cut : cut + TILE]
                atom_sums[matrix * 8 + atom, :9, :] += total

    def densities(tiles):
        def block(step, carry):
            value_copy(step).wait()
            reduce(jnp.maximum(step - 1, 0), step > 0)
            start = pl.multiple_of(step * BLOCK, BLOCK)
            columns = []
            for place in range(tiles):
                lane = pl.multiple_of(table[base + place] * TILE, TILE)
                columns.append(values_in[pl.ds(start, BLOCK), pl.ds(lane, TILE)])
            values = jnp.concatenate(columns, axis=1)
            sums = [None, None]
            for last in range(tiles):
                cols = slice(2 * last * TILE, (2 * last + 2) * TILE)
                down = (last + 1) * TILE
                both = jnp.concatenate(columns[: last + 1] + columns[:last], axis=1)
                got = jnp.dot(
                    both, parts[: (2 * last + 1) * TILE, cols], preferred_element_type=jnp.float32
                )
                column = columns[last].astype(jnp.float32)
                for matrix in range(2):
                    part = got[:, matrix * TILE : (matrix + 1) * TILE] * column
                    sums[matrix] = part if last == 0 else sums[matrix] + part
            for matrix in range(2):
                sums_kept[matrix] = sums[matrix]
            return carry

        lax.fori_loop(0, blocks, block, 0)

    for tiles in range(KT - 2, KT + 1):
        pl.when(count == tiles)(lambda tiles=tiles: densities(tiles))
    reduce(jnp.maximum(blocks - 1, 0), blocks > 0)

    density_copy = pltpu.make_async_copy(density, density_out, out_sems.at[0])
    density_copy.start()
    lane = lax.broadcasted_iota(jnp.int32, (9, TILE), 1)
    degree = lax.broadcasted_iota(jnp.int32, (9, TILE), 0)
    lane = lane - degree * SPAN - 4 * batch
    for matrix in range(2):
        total = jnp.zeros((9, TILE), jnp.float32)
        for atom in range(8):
            picked = jnp.sum(atom_sums[matrix * 8 + atom, :9, :], axis=1, keepdims=True)
            total = total + jnp.where(lane == atom, picked, 0.0)
        line = jnp.sum(total, axis=0, keepdims=True)
        if slot:
            line = line + before[matrix : matrix + 1, :]
            payload[:, matrix : matrix + 1, :] = jnp.broadcast_to(line[None], (DEVICES, 1, TILE))
        else:
            payload[matrix : matrix + 1, :] = line
    density_copy.wait()


def batch_call(slot, table, rows, carried, unit, offsets, weights, atoms, basis):
    arrays = [table, rows, *carried, unit, offsets, weights, atoms, basis]
    payload = (DEVICES, 2, TILE) if slot else (2, TILE)
    density = (2, 2, PTS) if slot else (2, PTS)
    own_rows = []
    if slot:
        own_rows = [
            pltpu.VMEM((DEVICES * PAIRS, TILE), jnp.int32),
            pltpu.SemaphoreType.DMA((4,)),
        ]

    def body(*refs):
        batch_body(slot, *refs)

    return pl.pallas_call(
        body,
        in_specs=[
            pl.BlockSpec(memory_space=pltpu.SMEM),
            pl.BlockSpec(memory_space=pltpu.HBM if slot else pltpu.VMEM),
            *[pl.BlockSpec(memory_space=pltpu.VMEM) for _ in arrays[2:-1]],
            pl.BlockSpec(memory_space=pltpu.HBM),
        ],
        out_specs=(
            pl.BlockSpec(memory_space=pl.ANY),
            pl.BlockSpec(memory_space=pltpu.VMEM),
        ),
        out_shape=(
            jax.ShapeDtypeStruct(density, jnp.float32),
            pltpu.VMEM(payload, jnp.float32),
        ),
        scratch_shapes=[
            pltpu.VMEM(((2 * KT - 1) * TILE, 2 * KT * TILE), jnp.bfloat16),
            pltpu.VMEM((PTS, KT * TILE), jnp.bfloat16),
            pltpu.VMEM(density, jnp.float32),
            pltpu.VMEM((2, BLOCK, TILE), jnp.float32),
            pltpu.VMEM((16, 16, TILE), jnp.float32),
            pltpu.SemaphoreType.DMA((STEPS,)),
            pltpu.SemaphoreType.DMA((1,)),
            *own_rows,
        ],
        compiler_params=pltpu.CompilerParams(vmem_limit_bytes=48 * 1024 * 1024),
        cost_estimate=pl.CostEstimate(
            flops=26_000_000_000, bytes_accessed=10_000_000, transcendentals=0
        ),
        name=f"batch_density_{slot}",
    )(*arrays)


def moment_body(arrived, out):
    lane = lax.broadcasted_iota(jnp.int32, (8, TILE), 1)
    for matrix in range(2):
        totals = [jnp.zeros((8, TILE), jnp.float32) for _ in range(9)]
        for place in range(16):
            part = arrived[pl.ds(2 * place + matrix, 8, stride=32), :]
            for degree in range(9):
                moved = pltpu.roll(part, (8 * place - SPAN * degree) % TILE, 1)
                if place < 15:
                    mine = (lane >= 8 * place) & (lane < 8 * place + SPAN)
                    totals[degree] = totals[degree] + jnp.where(mine, moved, 0.0)
                else:
                    inside = jnp.where(lane >= 8 * place, moved, 0.0)
                    after = pltpu.roll(jnp.where(lane < SPAN - 8, moved, 0.0), 1, 0)
                    totals[degree] = totals[degree] + inside + after
        for degree in range(9):
            for block in range(8):
                out[degree, matrix : matrix + 1, block * TILE : (block + 1) * TILE] = totals[degree][
                    block : block + 1, :
                ]


def moment_table(arrived):
    return pl.pallas_call(
        moment_body,
        out_shape=jax.ShapeDtypeStruct((9, 2, ATOMS), jnp.float32),
        in_specs=[pl.BlockSpec(memory_space=pltpu.VMEM)],
        out_specs=pl.BlockSpec(memory_space=pltpu.VMEM),
        compiler_params=pltpu.CompilerParams(vmem_limit_bytes=8 * 1024 * 1024),
        name="moment_table",
    )(arrived)


def exchange(value):
    return lax.all_to_all(value, ROW_COL, 0, 0, tiled=True)


def exchange_lines(rows):
    return exchange(rows.reshape(DEVICES, -1, 4, TILE)).reshape(-1, TILE)


def local(
    density_first,
    density_second,
    basis,
    tile_list,
    tile_count,
    point_count,
    offsets,
    weights,
    atom_of_point,
):
    rows = spread(tile_list, tile_count, point_count, density_first, density_second)
    rows = exchange_lines(rows)
    first, coded, starts, unit = windows(rows)
    first = exchange_lines(first)
    rest = exchange_lines(rest_windows(starts, coded))

    table = batch_tables(tile_list, tile_count, point_count)
    flat = basis.reshape(-1, KT * TILE)
    side = (unit, offsets, weights, atom_of_point)
    density_0, payload_0 = batch_call(0, table, first, (), *side, flat)
    density, payload = batch_call(
        1, table, rest, (payload_0, density_0), *side, flat
    )
    moments = moment_table(exchange(payload).reshape(DEVICES * 2, TILE)).swapaxes(0, 1)
    return density, moments


def solution(mesh):
    torus = Mesh(mesh.devices.reshape(4, 4, 4, 2), ("row_0", "row_1", "col_0", "col_1"))
    in_specs = (
        P(ROW, COL),
        P(ROW, COL),
        P(ROW_COL, None, None),
        P(ROW_COL, None),
        P(ROW_COL),
        P(ROW_COL),
        P(None, ROW_COL, None),
        P(ROW_COL, None),
        P(ROW_COL, None),
    )
    out_specs = (P(None, ROW_COL, None), P())
    return jax.shard_map(local, mesh=torus, in_specs=in_specs, out_specs=out_specs, check_vma=False)
```
